1024 devices in a mesh: gx: 4 (over x_hi, core), gy: 4 (over y), gz: 64 (over z, x_lo).
Axes of the slice: x: 4 (x_hi: 2, x_lo: 2; x = x_hi * 2 + x_lo), y: 4, z: 32, core: 2. Of those that a mesh axis runs over, the one named last changes fastest.
Arguments:
- velocity: float32 [3, 512, 16384], P(None, None, ('gx', 'gy', 'gz')), may hold values from -4 to 4
- inv_density: float32 [512, 16384], P(None, ('gx', 'gy', 'gz')), may hold values from 0.25 to 4
- element_place: int32 [16384], P(('gx', 'gy', 'gz')), may hold values from 0 to 15, as said below
Outputs:
- advected: float32 [3, 512, 16384], P(None, None, ('gx', 'gy', 'gz'))
- pressure: float32 [512, 16384], P(None, ('gx', 'gy', 'gz'))
- residual: float32 [512, 16384], P(None, ('gx', 'gy', 'gz'))
The draws below stay inside these ranges and needn't reach their ends.
Inputs may be any that keep to these rules, and one draw needn't show every extreme that they name: `element_place`: within each device's 16 consecutive elements every block position appears exactly once.
All inputs are finite; a program needn't handle non-finite values.
Results may differ from the reference program's by a relative error of at most 0.0003.
Values sent between devices are 32-bit elements; how exact they have to be, the bound alone decides.
No kernel may reach another device: no remote copies, remote signals or barrier semaphores. Data moves between devices by JAX's collectives and lax.ppermute only.
A program may use at most 32 MiB of HBM per device.

```python
import math
import jax
import jax.numpy as jnp
from jax import lax

PTS = 512
BX = 4
BY = 4
BZ = 1
CG_ITERS = 2
ELEM_DEV = 16
NEL = 16384
N_GX = 4
N_GY = 4
N_GZ = 64


def shuffle_block(block_key):
    return jax.random.permutation(block_key, ELEM_DEV)


def draw_element_place(key, part):
    devices = NEL // ELEM_DEV
    device_keys = jax.random.split(jax.random.fold_in(key, 17), devices)
    orders = jax.vmap(shuffle_block)(device_keys)
    return orders.reshape(NEL).astype(jnp.int32)


def block_levels(key, dims, cuts, least, high):
    def one(dim, parts):
        steps = jax.random.uniform(jax.random.fold_in(jax.random.fold_in(key, 6), dim), (parts,), jnp.float32, least / len(cuts), high / len(cuts))
        return jnp.repeat(jnp.exp(steps), dims[dim] // parts).reshape((-1,) + (1,) * (len(dims) - dim - 1))

    factor_of = one(*cuts[0])
    for cut in cuts[1:]:
        factor_of = factor_of * one(*cut)
    return factor_of


def scatter_about(rng, extent, deviation, most, cuts=(), kind=jnp.bfloat16):
    level = block_levels(rng, extent, cuts, -0.22, 0.18) if cuts else 1.0
    values = jax.random.normal(rng, extent, jnp.float32) * deviation * level
    return jnp.minimum(jnp.maximum(values, -most), most).astype(kind)


def setup_inputs(seed: int = 0) -> dict:
    key_of = jax.random.split(jax.random.key(seed), 4)
    velocity = scatter_about(key_of[0], (3, PTS, NEL), 1.0, 4.0, ((2, 1024),), jnp.float32)
    inv_density = jnp.clip(jnp.exp(math.log(4.0) - 2.7725887 * jax.random.uniform(key_of[1], (PTS, NEL), jnp.float32) ** block_levels(key_of[1], (PTS, NEL), ((1, 1024),), -0.2, 0.2)), 0.25, 4.0)
    element_place = draw_element_place(jax.random.fold_in(key_of[3], 71), 0)
    return dict(velocity=velocity, inv_density=inv_density, element_place=element_place)


time_step = 0.03
mass_shift = 4.0
contractions = ("ij,sjbce->sibce", "ij,sajce->saice", "ij,sabje->sabie")
inner_nodes = (-0.8717401485096066, -0.5917001814331423, -0.2092992179024789, 0.2092992179024789, 0.5917001814331423, 0.8717401485096066)


def legendre_seven(position):
    previous = 1.0
    current_value = position
    for degree_index in range(1, 7):
        following = ((2 * degree_index + 1) * position * current_value - degree_index * previous) / (degree_index + 1)
        previous = current_value
        current_value = following
    return current_value


def tables():
    node_values = [-1.0] + list(inner_nodes) + [1.0]
    poly_values = [legendre_seven(node) for node in node_values]
    weights = [2.0 / (56.0 * value * value) for value in poly_values]
    derivative = [[0.0] * 8 for row_index in range(8)]
    for row_index in range(8):
        for col_index in range(8):
            if row_index != col_index:
                derivative[row_index][col_index] = poly_values[row_index] / (poly_values[col_index] * (node_values[row_index] - node_values[col_index]))
    derivative[0][0] = -14.0
    derivative[7][7] = 14.0
    squared_t = [[derivative[col_index][row_index] ** 2 for col_index in range(8)] for row_index in range(8)]
    quad_list = [weights[first] * weights[second] * weights[third] for first in range(8) for second in range(8) for third in range(8)]
    quadrature = jnp.asarray(quad_list, jnp.float32).reshape(1, 8, 8, 8, 1)
    return (quadrature, jnp.asarray(derivative, jnp.float32), jnp.asarray(squared_t, jnp.float32))


def apply_along(matrix, values, direction):
    return jnp.einsum(contractions[direction], matrix, values, precision=lax.Precision.HIGHEST)


def multiplicity(offsets, totals, block_shape, elements):
    slot_index = jnp.arange(elements, dtype=jnp.int32)
    places = (slot_index // (block_shape[1] * block_shape[2]), slot_index // block_shape[2] % block_shape[1], slot_index % block_shape[2])
    node_index = jnp.arange(8, dtype=jnp.int32)
    first_node = (node_index == 0).astype(jnp.float32)[:, None]
    last_node = (node_index == 7).astype(jnp.float32)[:, None]
    factors = []
    for direction in range(3):
        position = places[direction] + offsets[direction]
        lower_open = (position > 0).astype(jnp.float32)[None, :]
        upper_open = (position < totals[direction] - 1).astype(jnp.float32)[None, :]
        factors.append(1.0 + first_node * lower_open + last_node * upper_open)
    joined = factors[0][:, None, None, :] * factors[1][None, :, None, :] * factors[2][None, None, :, :]
    return joined[None]


def assemble_axis(values, point_axis, grid_axis, block_shape, sender):
    lower_faces = lax.index_in_dim(values, 0, point_axis, keepdims=False)
    upper_faces = lax.index_in_dim(values, 7, point_axis, keepdims=False)
    flat_shape = lower_faces.shape
    grid_shape = flat_shape[:3] + tuple(block_shape)
    lower_faces = lower_faces.reshape(grid_shape)
    upper_faces = upper_faces.reshape(grid_shape)
    element_axis = 3 + grid_axis
    length = block_shape[grid_axis]
    interior = lax.slice_in_dim(upper_faces, 0, length - 1, axis=element_axis) + lax.slice_in_dim(lower_faces, 1, length, axis=element_axis)
    lower_edge = lax.slice_in_dim(lower_faces, 0, 1, axis=element_axis)
    upper_edge = lax.slice_in_dim(upper_faces, length - 1, length, axis=element_axis)
    arrived = sender(jnp.stack([lower_edge, upper_edge]))
    first_sum = lower_edge + arrived[0]
    last_sum = upper_edge + arrived[3]
    new_lower = jnp.concatenate([first_sum, interior], axis=element_axis).reshape(flat_shape)
    new_upper = jnp.concatenate([interior, last_sum], axis=element_axis).reshape(flat_shape)
    values = lax.dynamic_update_slice_in_dim(values, jnp.expand_dims(new_lower, point_axis), 0, point_axis)
    values = lax.dynamic_update_slice_in_dim(values, jnp.expand_dims(new_upper, point_axis), 7, point_axis)
    return values


def pad_sender(face_pair):
    return jnp.pad(face_pair, [(1, 1)] + [(0, 0)] * (face_pair.ndim - 1))


def invert_order(ordering):
    return jnp.zeros((ordering.shape[0],), jnp.int32).at[ordering].set(jnp.arange(ordering.shape[0], dtype=jnp.int32))


def to_grid(array, inverse, devices):
    leading = array.shape[:-1]
    rank_lead = len(leading)
    blocks = array.reshape(leading + (devices, ELEM_DEV))
    index_full = jnp.broadcast_to(inverse.reshape((1,) * rank_lead + (devices, ELEM_DEV)), blocks.shape)
    blocks = jnp.take_along_axis(blocks, index_full, axis=-1)
    blocks = blocks.reshape(leading + (N_GX, N_GY, N_GZ, BX, BY, BZ))
    axes_order = list(range(rank_lead)) + [rank_lead + 0, rank_lead + 3, rank_lead + 1, rank_lead + 4, rank_lead + 2, rank_lead + 5]
    return blocks.transpose(axes_order).reshape(leading + (-1,))


def from_grid(array, orders, devices):
    leading = array.shape[:-1]
    rank_lead = len(leading)
    blocks = array.reshape(leading + (N_GX, BX, N_GY, BY, N_GZ, BZ))
    axes_order = list(range(rank_lead)) + [rank_lead + 0, rank_lead + 2, rank_lead + 4, rank_lead + 1, rank_lead + 3, rank_lead + 5]
    blocks = blocks.transpose(axes_order).reshape(leading + (devices, ELEM_DEV))
    index_full = jnp.broadcast_to(orders.reshape((1,) * rank_lead + (devices, ELEM_DEV)), blocks.shape)
    return jnp.take_along_axis(blocks, index_full, axis=-1).reshape(leading + (-1,))


def reference(velocity, inv_density, element_place):
    devices = N_GX * N_GY * N_GZ
    grid_shape = (BX * N_GX, BY * N_GY, BZ * N_GZ)
    orders = element_place.reshape(devices, ELEM_DEV)
    inverse = jax.vmap(invert_order)(orders)
    quadrature, derivative, square_table = tables()
    advector = to_grid(velocity, inverse, devices).reshape(3, 8, 8, 8, -1)
    mobility = to_grid(inv_density, inverse, devices).reshape(1, 8, 8, 8, -1)
    elements = advector.shape[-1]
    copies = multiplicity((0, 0, 0), grid_shape, grid_shape, elements)
    mass = quadrature * copies
    inverse_copies = 1.0 / copies

    def assemble(values):
        values = assemble_axis(values, 1, 0, grid_shape, pad_sender)
        values = assemble_axis(values, 2, 1, grid_shape, pad_sender)
        return assemble_axis(values, 3, 2, grid_shape, pad_sender)

    def advection_rate(section_value):
        convective = advector[0:1] * apply_along(derivative, section_value, 0)
        convective = convective + advector[1:2] * apply_along(derivative, section_value, 1)
        convective = convective + advector[2:3] * apply_along(derivative, section_value, 2)
        return assemble(-quadrature * convective) / mass

    first_rate = advection_rate(advector)
    second_rate = advection_rate(advector + 0.5 * time_step * first_rate)
    third_rate = advection_rate(advector + 0.5 * time_step * second_rate)
    fourth_rate = advection_rate(advector + time_step * third_rate)
    advected = advector + (time_step / 6.0) * (first_rate + 2.0 * second_rate + 2.0 * third_rate + fourth_rate)

    divergence = apply_along(derivative, advected[0:1], 0) + apply_along(derivative, advected[1:2], 1) + apply_along(derivative, advected[2:3], 2)
    weighted = quadrature * mobility
    diag_local = mass_shift * quadrature + apply_along(square_table, weighted, 0) + apply_along(square_table, weighted, 1) + apply_along(square_table, weighted, 2)
    source_local = -quadrature * divergence / time_step
    assembled = assemble(jnp.concatenate([source_local, diag_local], axis=0))
    source = assembled[0:1]
    inverse_jacobi = 1.0 / assembled[1:2]

    def operator(values):
        summed = mass_shift * quadrature * values
        for direction in range(3):
            slope = apply_along(derivative, values, direction)
            summed = summed + apply_along(derivative.T, weighted * slope, direction)
        return assemble(summed)

    def inner(left, right):
        return jnp.sum(left * right * inverse_copies)

    pressure = jnp.zeros_like(source)
    residual = source
    precond = residual * inverse_jacobi
    search = precond
    current = inner(residual, precond)
    for iteration in range(CG_ITERS):
        applied = operator(search)
        step_size = current / inner(search, applied)
        pressure = pressure + step_size * search
        residual = residual - step_size * applied
        if iteration + 1 < CG_ITERS:
            precond = residual * inverse_jacobi
            following = inner(residual, precond)
            search = precond + (following / current) * search
            current = following
    advected_out = from_grid(advected.reshape(3, 512, -1), orders, devices)
    pressure_out = from_grid(pressure.reshape(512, -1), orders, devices)
    residual_out = from_grid(residual.reshape(512, -1), orders, devices)
    return advected_out, pressure_out, residual_out
```

```python
import jax
import jax.numpy as jnp
from jax import lax
from jax.sharding import Mesh
from jax.sharding import PartitionSpec as P

BX = 4
BY = 4
BZ = 1
CG_ITERS = 2
GX = ("gx_0", "gx_1")
GZ = ("gz_0", "gz_1")
GX_GY = ("gx_0", "gx_1", "gy")
GX_GY_GZ = ("gx_0", "gx_1", "gy", "gz_0", "gz_1")


time_step = 0.03
mass_shift = 4.0
inner_nodes = (
    -0.8717401485096066,
    -0.5917001814331423,
    -0.2092992179024789,
    0.2092992179024789,
    0.5917001814331423,
    0.8717401485096066,
)


def extended(cells, sides, width):
    for axis, dim in sides:
        count = lax.axis_size(axis)
        ends = count - 1
        head = lax.slice_in_dim(cells, 0, width, axis=dim)
        tail = lax.slice_in_dim(cells, cells.shape[dim] - width, cells.shape[dim], axis=dim)
        cells = jnp.concatenate(
            [
                lax.ppermute(tail, axis, [(i, (i + 1) % count) for i in range(ends)]),
                cells,
                lax.ppermute(head, axis, [((i + 1) % count, i) for i in range(ends)]),
            ],
            axis=dim,
        )
    return cells


def total(values):
    row = jnp.pad(jnp.stack(values), (0, 124)).reshape(1, 128)
    for axes in (GZ, GX_GY):
        count = lax.axis_size(axes)
        pieces = lax.all_to_all(jnp.broadcast_to(row[None], (count, 1, 128)), axes, 0, 0)
        row = jnp.sum(pieces, axis=0)
    return [row[0, index] for index in range(len(values))]


def legendre_seven(position):
    previous = 1.0
    current_value = position
    for degree_index in range(1, 7):
        following = (
            (2 * degree_index + 1) * position * current_value - degree_index * previous
        ) / (degree_index + 1)
        previous = current_value
        current_value = following
    return current_value


def tables():
    node_values = [-1.0] + list(inner_nodes) + [1.0]
    poly_values = [legendre_seven(node) for node in node_values]
    weights = [2.0 / (56.0 * value * value) for value in poly_values]
    derivative = [[0.0] * 8 for row_index in range(8)]
    for row_index in range(8):
        for col_index in range(8):
            if row_index != col_index:
                derivative[row_index][col_index] = poly_values[row_index] / (
                    poly_values[col_index] * (node_values[row_index] - node_values[col_index])
                )
    derivative[0][0] = -14.0
    derivative[7][7] = 14.0
    squared_t = [
        [derivative[col_index][row_index] ** 2 for col_index in range(8)] for row_index in range(8)
    ]
    quad_list = [
        weights[first] * weights[second] * weights[third]
        for first in range(8)
        for second in range(8)
        for third in range(8)
    ]
    quadrature = jnp.asarray(quad_list, jnp.float32).reshape(1, 8, 8, 8, 1)
    return (quadrature, jnp.asarray(derivative, jnp.float32), jnp.asarray(squared_t, jnp.float32))


def apply_along(matrix, widened, values, direction):
    if direction == 0:
        return jnp.einsum("ij,sjbk->sibk", matrix, values, precision=lax.Precision.HIGHEST)
    if direction == 1:
        return jnp.einsum("ij,sajk->saik", matrix, values, precision=lax.Precision.HIGHEST)
    return jnp.einsum("ij,sabj->sabi", widened, values, precision=lax.Precision.HIGHEST)


def multiplicity(offsets, totals, block_shape, elements):
    slot_index = jnp.arange(elements, dtype=jnp.int32)
    places = (
        slot_index // (block_shape[1] * block_shape[2]),
        slot_index // block_shape[2] % block_shape[1],
        slot_index % block_shape[2],
    )
    node_index = jnp.arange(8, dtype=jnp.int32)
    first_node = (node_index == 0).astype(jnp.float32)[:, None]
    last_node = (node_index == 7).astype(jnp.float32)[:, None]
    factors = []
    for direction in range(3):
        position = places[direction] + offsets[direction]
        lower_open = (position > 0).astype(jnp.float32)[None, :]
        upper_open = (position < totals[direction] - 1).astype(jnp.float32)[None, :]
        factors.append(1.0 + first_node * lower_open + last_node * upper_open)
    joined = (
        factors[0][:, None, None, :] * factors[1][None, :, None, :] * factors[2][None, None, :, :]
    )
    return joined[None]


def face_take(values, direction, node, block_shape):
    elements = block_shape[0] * block_shape[1] * block_shape[2]
    if direction == 2:
        piece = lax.slice_in_dim(values, node * elements, (node + 1) * elements, axis=3)
    else:
        piece = lax.index_in_dim(values, node, 1 + direction, keepdims=False).reshape(
            values.shape[0], 8, 8, elements
        )
    return piece.reshape(piece.shape[:3] + tuple(block_shape))


def face_write(values, direction, node, piece, elements):
    flat = piece.reshape(piece.shape[:3] + (elements,))
    if direction == 2:
        return lax.dynamic_update_slice_in_dim(values, flat, node * elements, 3)
    widened = jnp.expand_dims(flat.reshape(flat.shape[0], 8, 8 * elements), 1 + direction)
    return lax.dynamic_update_slice_in_dim(values, widened, node, 1 + direction)


def assemble_axis(values, direction, block_shape, sender):
    elements = block_shape[0] * block_shape[1] * block_shape[2]
    lower_faces = face_take(values, direction, 0, block_shape)
    upper_faces = face_take(values, direction, 7, block_shape)
    element_axis = 3 + direction
    length = block_shape[direction]
    interior = lax.slice_in_dim(upper_faces, 0, length - 1, axis=element_axis) + lax.slice_in_dim(
        lower_faces, 1, length, axis=element_axis
    )
    lower_edge = lax.slice_in_dim(lower_faces, 0, 1, axis=element_axis)
    upper_edge = lax.slice_in_dim(upper_faces, length - 1, length, axis=element_axis)
    arrived = sender(jnp.stack([lower_edge, upper_edge]))
    first_sum = lower_edge + arrived[0]
    last_sum = upper_edge + arrived[3]
    new_lower = jnp.concatenate([first_sum, interior], axis=element_axis)
    new_upper = jnp.concatenate([interior, last_sum], axis=element_axis)
    values = face_write(values, direction, 0, new_lower, elements)
    return face_write(values, direction, 7, new_upper, elements)


def send_along_x(face_pair):
    return extended(face_pair, ((GX, 0),), 1)


def send_along_y(face_pair):
    return extended(face_pair, (("gy", 0),), 1)


def send_along_z(face_pair):
    return extended(face_pair, ((GZ, 0),), 1)


def assemble(values):
    block_shape = (BX, BY, BZ)
    values = assemble_axis(values, 0, block_shape, send_along_x)
    values = assemble_axis(values, 1, block_shape, send_along_y)
    return assemble_axis(values, 2, block_shape, send_along_z)


def per_device(velocity, inv_density, element_place):
    elements = element_place.shape[0]
    width = 8 * elements
    quadrature, derivative, square_table = tables()
    identity = jnp.eye(elements, dtype=jnp.float32)
    derivative_wide = jnp.kron(derivative, identity)
    transpose_wide = jnp.kron(derivative.T, identity)
    square_wide = jnp.kron(square_table, identity)
    slot_index = jnp.arange(elements, dtype=jnp.int32)
    inverse = jnp.zeros((elements,), jnp.int32).at[element_place].set(slot_index)
    advector = jnp.take(velocity, inverse, axis=2).reshape(3, 8, 8, width)
    mobility = jnp.take(inv_density, inverse, axis=1).reshape(1, 8, 8, width)
    quad_wide = jnp.broadcast_to(quadrature, (1, 8, 8, 8, elements)).reshape(1, 8, 8, width)
    offsets = (lax.axis_index(GX) * BX, lax.axis_index("gy") * BY, lax.axis_index(GZ) * BZ)
    totals = (BX * lax.axis_size(GX), BY * lax.axis_size("gy"), BZ * lax.axis_size(GZ))
    copies = multiplicity(offsets, totals, (BX, BY, BZ), elements).reshape(1, 8, 8, width)
    mass = quad_wide * copies
    inverse_copies = 1.0 / copies

    def advection_rate(section_value):
        convective = advector[0:1] * apply_along(derivative, derivative_wide, section_value, 0)
        convective = convective + advector[1:2] * apply_along(
            derivative, derivative_wide, section_value, 1
        )
        convective = convective + advector[2:3] * apply_along(
            derivative, derivative_wide, section_value, 2
        )
        return assemble(-quad_wide * convective) / mass

    first_rate = advection_rate(advector)
    second_rate = advection_rate(advector + 0.5 * time_step * first_rate)
    third_rate = advection_rate(advector + 0.5 * time_step * second_rate)
    fourth_rate = advection_rate(advector + time_step * third_rate)
    advected = advector + time_step / 6.0 * (
        first_rate + 2.0 * second_rate + 2.0 * third_rate + fourth_rate
    )
    divergence = (
        apply_along(derivative, derivative_wide, advected[0:1], 0)
        + apply_along(derivative, derivative_wide, advected[1:2], 1)
        + apply_along(derivative, derivative_wide, advected[2:3], 2)
    )
    weighted = quad_wide * mobility
    diag_local = (
        mass_shift * quad_wide
        + apply_along(square_table, square_wide, weighted, 0)
        + apply_along(square_table, square_wide, weighted, 1)
        + apply_along(square_table, square_wide, weighted, 2)
    )
    source_local = -quad_wide * divergence / time_step
    assembled = assemble(jnp.concatenate([source_local, diag_local], axis=0))
    source = assembled[0:1]
    inverse_jacobi = 1.0 / assembled[1:2]

    def operator(values):
        summed = mass_shift * quad_wide * values
        for direction in range(3):
            slope = apply_along(derivative, derivative_wide, values, direction)
            summed = summed + apply_along(derivative.T, transpose_wide, weighted * slope, direction)
        return assemble(summed)

    first = source * inverse_jacobi
    first_applied = operator(first)
    second = first_applied * inverse_jacobi
    second_applied = operator(second)
    rho, curvature, cross, last = total(
        [
            jnp.sum(source * first * inverse_copies),
            jnp.sum(first * first_applied * inverse_copies),
            jnp.sum(first_applied * second * inverse_copies),
            jnp.sum(second * second_applied * inverse_copies),
        ]
    )
    step = rho / curvature
    rho_next = step * step * cross - rho
    ratio = rho_next / rho
    step_next = rho_next / (
        curvature - 2.0 * step * cross + step * step * last - ratio * ratio * curvature
    )
    keep = step + step_next * (1.0 + ratio)
    pressure = keep * first - step_next * step * second
    residual = source - keep * first_applied + step_next * step * second_applied
    advected_out = jnp.take(advected.reshape(3, 512, elements), element_place, axis=2)
    pressure_out = jnp.take(pressure.reshape(512, elements), element_place, axis=1)
    residual_out = jnp.take(residual.reshape(512, elements), element_place, axis=1)
    return (advected_out, pressure_out, residual_out)


def solution(mesh):
    torus = Mesh(
        mesh.devices.reshape(2, 2, mesh.shape["gy"], 32, 2), ("gx_0", "gx_1", "gy", "gz_0", "gz_1")
    )
    placed = (P(None, None, GX_GY_GZ), P(None, GX_GY_GZ), P(GX_GY_GZ))
    return jax.shard_map(
        per_device,
        mesh=torus,
        in_specs=placed,
        out_specs=(P(None, None, GX_GY_GZ), P(None, GX_GY_GZ), P(None, GX_GY_GZ)),
        check_vma=False,
    )
```

```python
import jax
import jax.numpy as jnp
from jax import lax
from jax.experimental import pallas as pl
from jax.experimental.pallas import tpu as pltpu
from jax.sharding import Mesh
from jax.sharding import PartitionSpec as P

GX = ("gx_0", "gx_1")
GZ = ("gz_0", "gz_1")
GX_GY = ("gx_0", "gx_1", "gy")
GX_GY_GZ = ("gx_0", "gx_1", "gy", "gz_0", "gz_1")
F32 = jnp.float32
PTS = 512
LANES = 128

time_step = 0.03
mass_shift = 4.0
inner_nodes = (
    -0.8717401485096066,
    -0.5917001814331423,
    -0.2092992179024789,
    0.2092992179024789,
    0.5917001814331423,
    0.8717401485096066,
)


def legendre_seven(position):
    previous = 1.0
    current_value = position
    for degree_index in range(1, 7):
        following = (
            (2 * degree_index + 1) * position * current_value - degree_index * previous
        ) / (degree_index + 1)
        previous = current_value
        current_value = following
    return current_value


def tables():
    nodes = [-1.0] + list(inner_nodes) + [1.0]
    poly = [legendre_seven(node) for node in nodes]
    weights = [2.0 / (56.0 * value * value) for value in poly]
    deriv = [[0.0] * 8 for _ in range(8)]
    for i in range(8):
        for j in range(8):
            if i != j:
                deriv[i][j] = poly[i] / (poly[j] * (nodes[i] - nodes[j]))
    deriv[0][0] = -14.0
    deriv[7][7] = 14.0
    return weights, deriv


WEIGHTS, DERIV = tables()
DERIV_T = [[DERIV[j][i] for j in range(8)] for i in range(8)]
SQUARE = [[DERIV[j][i] ** 2 for j in range(8)] for i in range(8)]
MINUS = [[-DERIV[i][j] for j in range(8)] for i in range(8)]


def mix(matrix, values, which=range(8)):
    out = []
    for i in which:
        total_value = None
        for j in range(8):
            if matrix[i][j] != 0.0:
                term = matrix[i][j] * values[j]
                total_value = term if total_value is None else total_value + term
        out.append(total_value)
    return out


def columns(matrix):
    sub = lax.broadcasted_iota(jnp.int32, (8, LANES), 0)
    out = []
    for j in range(8):
        col = jnp.zeros((8, LANES), F32)
        for i in range(8):
            col = jnp.where(sub == i, F32(matrix[i][j]), col)
        out.append(col)
    return out


def weight_column():
    sub = lax.broadcasted_iota(jnp.int32, (8, LANES), 0)
    col = jnp.zeros((8, LANES), F32)
    for i in range(8):
        col = jnp.where(sub == i, F32(WEIGHTS[i]), col)
    return col


def rows8(start):
    return pl.ds(pl.multiple_of(start, 8), 8)


def mix_inner(cols, ref, lead, start):
    total_value = None
    for j in range(8):
        term = cols[j] * ref[lead + (pl.ds(start + j, 8, stride=0), slice(None))]
        total_value = term if total_value is None else total_value + term
    return total_value


def place_of(tile):
    lane = lax.broadcasted_iota(jnp.int32, (1, LANES), 1)
    block = lane >> 4
    if tile == 0:
        row = block + 2
    else:
        row = jnp.where(block == 0, 1, jnp.where(block == 1, 10, jnp.where(block == 2, 0, 11)))
    return lane, block, lane & 15, row + 4 * (lax.axis_index("gy") - 1)


def pair_weights(has_low, has_high, average):
    own, other = (0.5, 0.5) if average else (1.0, 1.0)
    return (
        jnp.where(has_low, F32(own), F32(1.0)),
        jnp.where(has_low, F32(other), F32(0.0)),
        jnp.where(has_high, F32(own), F32(1.0)),
        jnp.where(has_high, F32(other), F32(0.0)),
    )


def x_weights(average):
    _, _, ix, _ = place_of(0)
    return pair_weights(ix > 0, ix < 15, average)


def y_weights(tile, average):
    _, _, _, y = place_of(tile)
    return pair_weights(y > 0, y < 4 * lax.axis_size("gy") - 1, average)


def z_index():
    return lax.axis_index("gz_0") * lax.axis_size("gz_1") + lax.axis_index("gz_1")


def z_weights():
    z = jnp.full((1, LANES), z_index(), jnp.int32)
    return pair_weights(z > 0, z < lax.axis_size("gz_0") * lax.axis_size("gz_1") - 1, True)


def roll(x, shift):
    return pltpu.roll(x, shift % LANES, 1)


def x_join(ref, lead, w):
    low, high = lead + (slice(0, 64),), lead + (slice(448, 512),)
    f0, f7 = ref[low], ref[high]
    ref[low] = w[0] * f0 + w[1] * roll(f7, 1)
    ref[high] = w[2] * f7 + w[3] * roll(f0, -1)


def y_join(ref, lead, w):
    for a in range(8):
        low, high = lead + (slice(64 * a, 64 * a + 8),), lead + (slice(64 * a + 56, 64 * a + 64),)
        f0, f7 = ref[low], ref[high]
        ref[low] = w[0] * f0 + w[1] * roll(f7, 16)
        ref[high] = w[2] * f7 + w[3] * roll(f0, -16)


def y_join_two(ref, far, lead, w, far_w):
    lane, block, _, _ = place_of(0)
    for a in range(8):
        low, high = lead + (slice(64 * a, 64 * a + 8),), lead + (slice(64 * a + 56, 64 * a + 64),)
        f0, f7, g0, g7 = ref[low], ref[high], far[low], far[high]
        below = jnp.where(block == 0, g7, roll(f7, 16))
        above = jnp.where(block == 7, roll(g0, -32), roll(f0, -16))
        ref[low] = w[0] * f0 + w[1] * below
        ref[high] = w[2] * f7 + w[3] * above
        if far_w is not None:
            below = jnp.where(block == 0, roll(g7, -32), roll(f7, 32))
            above = jnp.where(block == 0, f0, roll(g0, -32))
            far[low] = far_w[0] * g0 + far_w[1] * below
            far[high] = far_w[2] * g7 + far_w[3] * above


def face(ref, lead, c):
    return ref[lead + (pl.ds(c, 64, stride=8), slice(None))]


def set_face(ref, lead, c, value):
    ref[lead + (pl.ds(c, 64, stride=8), slice(None))] = value


def convect(i, v, vel, out, minus_cols):
    def along_a(b, carry):
        start = 8 * b
        got = mix(MINUS, [v[i, rows8(64 * a + start)] for a in range(8)])
        for a in range(8):
            at = rows8(64 * a + start)
            out[i, at] = vel[0, at] * got[a]
        return carry

    lax.fori_loop(0, 8, along_a, 0)

    def along_bc(a, carry):
        start = 64 * a
        got = mix(MINUS, [v[i, rows8(start + 8 * b)] for b in range(8)])
        for b in range(8):
            at = rows8(start + 8 * b)
            inner = mix_inner(minus_cols, v, (i,), start + 8 * b)
            out[i, at] = out[i, at] + (vel[1, at] * got[b] + vel[2, at] * inner)
        return carry

    lax.fori_loop(0, 8, along_bc, 0)


def convect_y_faces(i, v, vel, out, minus_cols):
    for b in (0, 7):
        got = mix(MINUS, [v[i, slice(64 * a + 8 * b, 64 * a + 8 * b + 8)] for a in range(8)])
        for a in range(8):
            at = slice(64 * a + 8 * b, 64 * a + 8 * b + 8)
            out[i, at] = vel[0, at] * got[a]

    def along_bc(a, carry):
        start = 64 * a
        got = mix(MINUS, [v[i, rows8(start + 8 * b)] for b in range(8)], (0, 7))
        for b, value in zip((0, 7), got):
            at = rows8(start + 8 * b)
            inner = mix_inner(minus_cols, v, (i,), start + 8 * b)
            out[i, at] = out[i, at] + (vel[1, at] * value + vel[2, at] * inner)
        return carry

    lax.fori_loop(0, 8, along_bc, 0)


def pack_kernel(place, vel, inv, out):
    def move(s, carry):
        q = place[s]
        r = (q % 4) * 4 + q // 4
        for i in range(3):
            out[i, pl.ds(r, 1), :] = vel[i, pl.ds(s, 1), :]
        out[3, pl.ds(r, 1), :] = inv[pl.ds(s, 1), :]
        return carry

    lax.fori_loop(0, 16, move, 0)


FAR_ROWS = (1, 10, 0, 11)


def unpack(got, i, near, far, scratch, lead):
    for r in range(12):
        base = 16 * (r - 2) if 2 <= r <= 9 else LANES + 16 * FAR_ROWS.index(r)
        for g in range(4):
            first = 4 * (r % 4)
            scratch[slice(base + 4 * g, base + 4 * g + 4), :] = got[
                g, r // 4, i, slice(first, first + 4), :
            ]
    for p in range(4):
        at = slice(128 * p, 128 * p + 128)
        near[lead + (at,)] = jnp.transpose(scratch[0:128, at])
        far[lead + (at,)] = jnp.transpose(scratch[128:256, at])


def first_kernel(got, vel, vel_far, rate, rate_far, up, down, inv, inv_far, scratch):
    scratch[192:256, :] = jnp.zeros((64, PTS), F32)
    for i in range(3):
        unpack(got, i, vel, vel_far, scratch, (i,))
    unpack(got, 3, inv, inv_far, scratch, ())
    minus_cols = columns(MINUS)
    xw = x_weights(True)
    yw = y_weights(0, True)
    fw = y_weights(1, True)

    def component(i, carry):
        convect(i, vel, vel, rate, minus_cols)
        convect(i, vel_far, vel_far, rate_far, minus_cols)
        x_join(rate, (i,), xw)
        x_join(rate_far, (i,), xw)
        y_join_two(rate, rate_far, (i,), yw, fw)
        return carry

    lax.fori_loop(0, 3, component, 0)
    lane, _, _, _ = place_of(0)
    for c, out in ((7, up), (0, down)):
        for i in range(3):
            out[slice(64 * i, 64 * i + 64), :] = face(rate, (i,), c)
        far = [face(rate_far, (i,), c) for i in range(3)]
        out[192:256, :] = jnp.where(
            lane < 32, far[0], jnp.where(lane < 64, roll(far[1], 32), roll(far[2], 64))
        )


def advance(vel, rate, below, above, acc_in, scale, acc_scale, v, acc):
    zw = z_weights()

    def step(k, carry):
        at = rows8(8 * k)
        for i in range(3):
            r = rate[i, at]
            v[i, at] = vel[i, at] + scale * r
            if acc is not None:
                acc[i, at] = acc_in[i, at] + acc_scale * r
        return carry

    lax.fori_loop(0, 64, step, 0, unroll=2)
    for i in range(3):
        for c, got, own, other in ((0, below, zw[0], zw[1]), (7, above, zw[2], zw[3])):
            k = own * face(rate, (i,), c) + other * got[i]
            set_face(v, (i,), c, face(vel, (i,), c) + scale * k)
            if acc is not None:
                set_face(acc, (i,), c, face(acc_in, (i,), c) + acc_scale * k)


def thirds(ref):
    return [ref[slice(64 * i, 64 * i + 64), :] for i in range(3)]


def second_kernel(
    vel, vel_far, rate, rate_far, below, above, acc, out, up, down, v, v_far, out_far
):
    advance(
        vel, rate, thirds(below), thirds(above), vel, 0.5 * time_step, time_step / 6.0, v, acc
    )
    far = [[roll(ref[192:256, :], -32 * i) for i in range(3)] for ref in (below, above)]
    advance(vel_far, rate_far, far[0], far[1], None, 0.5 * time_step, 0.0, v_far, None)
    minus_cols = columns(MINUS)
    xw = x_weights(True)
    yw = y_weights(0, True)

    def component(i, carry):
        convect(i, v, vel, out, minus_cols)
        convect_y_faces(i, v_far, vel_far, out_far, minus_cols)
        x_join(out, (i,), xw)
        x_join_faces(out_far, i, xw)
        y_join_two(out, out_far, (i,), yw, None)
        return carry

    lax.fori_loop(0, 3, component, 0)
    send_faces(out, up, down)


def x_join_faces(ref, i, w):
    for b in (0, 7):
        low, high = slice(8 * b, 8 * b + 8), slice(448 + 8 * b, 448 + 8 * b + 8)
        f0, f7 = ref[i, low], ref[i, high]
        ref[i, low] = w[0] * f0 + w[1] * roll(f7, 1)
        ref[i, high] = w[2] * f7 + w[3] * roll(f0, -1)


def send_faces(rate, up, down):
    for i in range(3):
        up[slice(64 * i, 64 * i + 64), :] = face(rate, (i,), 7)
        down[slice(64 * i, 64 * i + 64), :] = face(rate, (i,), 0)


def stage_kernel(scale, acc_scale):
    def kernel(vel, acc_in, rate, below, above, acc, out, up, down, v):
        advance(vel, rate, thirds(below), thirds(above), acc_in, scale, acc_scale, v, acc)
        minus_cols = columns(MINUS)
        xw = x_weights(True)
        yw = y_weights(0, True)

        def component(i, carry):
            convect(i, v, vel, out, minus_cols)
            x_join(out, (i,), xw)
            y_join(out, (i,), yw)
            return carry

        lax.fori_loop(0, 3, component, 0)
        send_faces(out, up, down)

    return kernel


def own_rows():
    _, block, _, _ = place_of(0)
    return block


def source_kernel(acc_in, rate, below, above, advected, source, up, down, joined):
    advance(acc_in, rate, thirds(below), thirds(above), None, time_step / 6.0, 0.0, advected, None)
    cols = columns(DERIV)
    wc = weight_column()

    def along_a(b, carry):
        start = 8 * b
        got = mix(DERIV, [advected[0, rows8(64 * a + start)] for a in range(8)])
        for a in range(8):
            source[rows8(64 * a + start)] = got[a]
        return carry

    lax.fori_loop(0, 8, along_a, 0)
    for a in range(8):
        start = 64 * a
        got = mix(DERIV, [advected[1, slice(start + 8 * b, start + 8 * b + 8)] for b in range(8)])
        for b in range(8):
            at = slice(start + 8 * b, start + 8 * b + 8)
            inner = mix_inner(cols, advected, (2,), start + 8 * b)
            scale = -WEIGHTS[a] * WEIGHTS[b] / time_step
            source[at] = (source[at] + got[b] + inner) * (scale * wc)
    joined[...] = source[...]
    block = own_rows()
    take_low = jnp.where((block >= 3) & (block <= 5), F32(1.0), F32(0.0))
    take_high = jnp.where((block >= 2) & (block <= 4), F32(1.0), F32(0.0))
    y_join(joined, (), (1.0, take_low, 1.0, take_high))
    lane, _, _, _ = place_of(0)
    for out, first in ((down, 1), (up, 2)):
        total_value = None
        for q in range(4):
            part = roll(joined[slice(128 * q, 128 * q + 128), :], 32 * (q - first))
            total_value = part if q == 0 else jnp.where(lane >> 5 == q, part, total_value)
        out[...] = total_value


def spread_kernel(joined, below, above, full, up, down):
    lane, block, _, _ = place_of(0)
    for q in range(4):
        at = slice(128 * q, 128 * q + 128)
        full[at, :] = jnp.where(
            lane < 32,
            roll(below[...], -32 * q),
            jnp.where(lane >= 96, roll(above[...], 96 - 32 * q), joined[at, :]),
        )
    take_low = jnp.where((block == 2) | (block == 6), F32(1.0), F32(0.0))
    take_high = jnp.where((block == 1) | (block == 5), F32(1.0), F32(0.0))
    y_join(full, (), (1.0, take_low, 1.0, take_high))
    x_join(full, (), x_weights(False))
    up[...] = face(full, (), 7)
    down[...] = face(full, (), 0)


def diagonal_kernel(inv, inv_far, weighted, diag, up, down, weighted_far, diag_far):
    wc = weight_column()
    cols = columns(SQUARE)
    for a in range(8):
        for b in range(8):
            at = slice(64 * a + 8 * b, 64 * a + 8 * b + 8)
            scale = WEIGHTS[a] * WEIGHTS[b] * wc
            weighted[at] = scale * inv[at]
            weighted_far[at] = scale * inv_far[at]
    for src, out, bs in ((weighted, diag, range(8)), (weighted_far, diag_far, (0, 7))):
        for b in bs:
            got = mix(SQUARE, [src[slice(64 * a + 8 * b, 64 * a + 8 * b + 8)] for a in range(8)])
            for a in range(8):
                out[slice(64 * a + 8 * b, 64 * a + 8 * b + 8)] = got[a]
        for a in range(8):
            start = 64 * a
            got = mix(SQUARE, [src[slice(start + 8 * b, start + 8 * b + 8)] for b in range(8)], bs)
            for b, value in zip(bs, got):
                at = slice(start + 8 * b, start + 8 * b + 8)
                inner = mix_inner(cols, src, (), start + 8 * b)
                scale = mass_shift * WEIGHTS[a] * WEIGHTS[b]
                out[at] = out[at] + value + inner + scale * wc
    xw = x_weights(False)
    x_join(diag, (), xw)
    for b in (0, 7):
        low, high = slice(8 * b, 8 * b + 8), slice(448 + 8 * b, 448 + 8 * b + 8)
        f0, f7 = diag_far[low], diag_far[high]
        diag_far[low] = xw[0] * f0 + xw[1] * roll(f7, 1)
        diag_far[high] = xw[2] * f7 + xw[3] * roll(f0, -1)
    y_join_two(diag, diag_far, (), y_weights(0, False), None)
    up[...] = face(diag, (), 7)
    down[...] = face(diag, (), 0)


def z_sum(src, below, above, dst):
    dst[...] = src[...]
    set_face(dst, (), 0, face(src, (), 0) + below)
    set_face(dst, (), 7, face(src, (), 7) + above)


def operate(u, weighted, out, flux):
    cols = columns(DERIV)
    cols_t = columns(DERIV_T)
    _, _, _, y = place_of(0)
    inside = (y >= 0) & (y < 4 * lax.axis_size("gy"))
    wc = jnp.where(inside, weight_column(), F32(0.0))

    def along_a(b, carry):
        start = 8 * b
        at = [rows8(64 * a + start) for a in range(8)]
        slope = mix(DERIV, [u[at[a]] for a in range(8)])
        got = mix(DERIV_T, [weighted[at[a]] * slope[a] for a in range(8)])
        for a in range(8):
            out[at[a]] = got[a]
        return carry

    lax.fori_loop(0, 8, along_a, 0)

    for a in range(8):
        start = 64 * a
        at = [slice(start + 8 * b, start + 8 * b + 8) for b in range(8)]
        values = [u[at[b]] for b in range(8)]
        weights = [weighted[at[b]] for b in range(8)]
        slope = mix(DERIV, values)
        got = mix(DERIV_T, [weights[b] * slope[b] for b in range(8)])
        for b in range(8):
            flux[at[b]] = weights[b] * mix_inner(cols, u, (), start + 8 * b)
            scale = mass_shift * WEIGHTS[a] * WEIGHTS[b]
            out[at[b]] = out[at[b]] + (got[b] + (scale * wc) * values[b])

    def along_c(k, carry):
        at = rows8(8 * k)
        out[at] = out[at] + mix_inner(cols_t, flux, (), 8 * k)
        return carry

    lax.fori_loop(0, 64, along_c, 0, unroll=4)


def own_mask():
    _, block, ix, _ = place_of(0)
    gx = lax.axis_index("gx_0") * lax.axis_size("gx_1") + lax.axis_index("gx_1")
    return jnp.where((block >= 2) & (block <= 5) & ((ix >> 2) == gx), F32(1.0), F32(0.0))


def dot(left, right):
    def step(k, carry):
        at = rows8(8 * k)
        return carry + left[at] * right[at]

    return lax.fori_loop(0, 64, step, jnp.zeros((8, LANES), F32), unroll=8)


def operator_one_kernel(
    partial, below, above, diag, diag_below, diag_above, source, weighted,
    residual, inverse, first, local, out, up, down, sums, flux,
):
    z_sum(partial, below[...], above[...], residual)
    z_sum(diag, diag_below[...], diag_above[...], inverse)
    inverse[...] = 1.0 / inverse[...]
    first[...] = residual[...] * inverse[...]
    operate(first, weighted, local, flux)
    out[...] = local[...]
    x_join(out, (), x_weights(False))
    y_join(out, (), y_weights(0, False))
    up[...] = face(out, (), 7)
    down[...] = face(out, (), 0)
    sums[0] = dot(source, first)
    sums[1] = dot(local, first)


def operator_two_kernel(
    partial, below, above, inverse, weighted, local, sums,
    applied, second, out, up, down, totals, local_two, flux,
):
    z_sum(partial, below[...], above[...], applied)
    second[...] = applied[...] * inverse[...]
    operate(second, weighted, local_two, flux)
    mask = own_mask()
    lane = lax.broadcasted_iota(jnp.int32, (1, LANES), 1)
    row = jnp.zeros((1, LANES), F32)
    for k, value in enumerate((sums[0], sums[1], dot(local, second), dot(local_two, second))):
        part = jnp.sum(mask * value, axis=0, keepdims=True)
        part = jnp.sum(part, axis=1, keepdims=True)
        row = jnp.where(lane == k, part, row)
    totals[...] = row
    out[...] = local_two[...]
    x_join(out, (), x_weights(False))
    y_join(out, (), y_weights(0, False))
    up[...] = face(out, (), 7)
    down[...] = face(out, (), 0)


def to_slots(place, ref, lead, out, k, scratch):
    for p in range(4):
        at = slice(128 * p, 128 * p + 128)
        scratch[:, at] = jnp.transpose(ref[lead + (at,)])
    gx = lax.axis_index("gx_0") * lax.axis_size("gx_1") + lax.axis_index("gx_1")
    for s in range(16):
        q = place[s]
        lane = (2 + q % 4) * 16 + 4 * gx + q // 4
        out[k, slice(s, s + 1), :] = scratch[pl.ds(lane, 1), :]


def advected_kernel(place, advected, out, scratch):
    for i in range(3):
        to_slots(place, advected, (i,), out, i, scratch)


def fields_kernel(place, residual, first, applied, second, out, scratch):
    for k, ref in enumerate((residual, first, applied, second)):
        to_slots(place, ref, (), out, k, scratch)


def last_kernel(place, partial, below, above, out, full, scratch):
    z_sum(partial, below[...], above[...], full)
    to_slots(place, full, (), out, 0, scratch)


def call(kernel, outs, scratch=(), scalars=0):
    def run(*args):
        vm = pl.BlockSpec(memory_space=pltpu.VMEM)
        sm = pl.BlockSpec(memory_space=pltpu.SMEM)
        result = pl.pallas_call(
            kernel,
            out_shape=tuple(jax.ShapeDtypeStruct(shape, F32) for shape in outs),
            in_specs=[sm] * scalars + [vm] * (len(args) - scalars),
            out_specs=tuple(vm for _ in outs),
            scratch_shapes=[pltpu.VMEM(shape, F32) for shape in scratch],
        )(*args)
        return result

    return run


def shift(values, axis, step):
    count = lax.axis_size(axis)
    pairs = [(i, i + step) for i in range(count) if 0 <= i + step < count]
    return lax.ppermute(values, axis, pairs)


def along(axis, up, down):
    return shift(up, axis, 1), shift(down, axis, -1)


def total(row):
    for axes in (GX_GY, GZ):
        count = lax.axis_size(axes)
        pieces = lax.all_to_all(jnp.broadcast_to(row[None], (count, 1, 128)), axes, 0, 0)
        row = jnp.sum(pieces, axis=0)
    return row


FULL = (PTS, LANES)
THREE = (3, PTS, LANES)
FACE = (64, LANES)


def per_device(velocity, inv_density, element_place):
    by_slot = jnp.transpose(velocity, (0, 2, 1))
    inv_slot = jnp.transpose(inv_density)
    (block,) = call(pack_kernel, [(4, 16, PTS)], scalars=1)(element_place, by_slot, inv_slot)
    below, above = along("gy", block, block)
    got = lax.all_gather(jnp.stack([below, block, above]), GX)
    vel, vel_far, rate, rate_far, up, down, inv, inv_far = call(
        first_kernel,
        [THREE, THREE, THREE, THREE, (256, LANES), (256, LANES), FULL, FULL],
        [(256, PTS)],
    )(got)
    below, above = along(GZ, up, down)
    weighted, diag, diag_up, diag_down = call(
        diagonal_kernel, [FULL, FULL, FACE, FACE], [FULL, FULL]
    )(inv, inv_far)
    acc, rate, up, down = call(
        second_kernel, [THREE, THREE, (192, LANES), (192, LANES)], [THREE, THREE, THREE]
    )(vel, vel_far, rate, rate_far, below, above)
    for scale in (0.5 * time_step, time_step):
        below, above = along(GZ, up, down)
        acc, rate, up, down = call(
            stage_kernel(scale, time_step / 3.0),
            [THREE, THREE, (192, LANES), (192, LANES)],
            [THREE],
        )(vel, acc, rate, below, above)
    below, above = along(GZ, up, down)
    advected, source, up, down, joined = call(
        source_kernel, [THREE, FULL, (128, LANES), (128, LANES), FULL]
    )(acc, rate, below, above)
    below, above = along("gy", up, down)
    (advected_slots,) = call(advected_kernel, [(3, 16, PTS)], [(LANES, PTS)], 1)(
        element_place, advected
    )
    full, up, down = call(spread_kernel, [FULL, FACE, FACE])(joined, below, above)
    below, above = along(
        GZ, jnp.concatenate([up, diag_up]), jnp.concatenate([down, diag_down])
    )
    residual, inverse, first, local, partial, up, down, sums = call(
        operator_one_kernel, [FULL, FULL, FULL, FULL, FULL, FACE, FACE, (2, 8, LANES)], [FULL]
    )(full, below[:64], above[:64], diag, below[64:], above[64:], source, weighted)
    below, above = along(GZ, up, down)
    applied, second, partial, up, down, totals = call(
        operator_two_kernel, [FULL, FULL, FULL, FACE, FACE, (1, LANES)], [FULL, FULL]
    )(partial, below, above, inverse, weighted, local, sums)
    below, above = along(GZ, up, down)
    sums = total(totals)
    (fields,) = call(fields_kernel, [(4, 16, PTS)], [(LANES, PTS)], 1)(
        element_place, residual, first, applied, second
    )
    (last,) = call(last_kernel, [(1, 16, PTS)], [FULL, (LANES, PTS)], 1)(
        element_place, partial, below, above
    )
    rho, curvature, cross, tail = sums[0, 0], sums[0, 1], sums[0, 2], sums[0, 3]
    step = rho / curvature
    rho_next = step * step * cross - rho
    ratio = rho_next / rho
    step_next = rho_next / (
        curvature - 2.0 * step * cross + step * step * tail - ratio * ratio * curvature
    )
    keep = step + step_next * (1.0 + ratio)
    pressure = keep * fields[1] - step_next * step * fields[3]
    residual = fields[0] - keep * fields[2] + step_next * step * last[0]
    return (
        jnp.transpose(advected_slots, (0, 2, 1)),
        jnp.transpose(pressure),
        jnp.transpose(residual),
    )


def solution(mesh):
    torus = Mesh(
        mesh.devices.reshape(2, 2, mesh.shape["gy"], -1, 2),
        ("gx_0", "gx_1", "gy", "gz_0", "gz_1"),
    )
    placed = (P(None, None, GX_GY_GZ), P(None, GX_GY_GZ), P(GX_GY_GZ))
    return jax.shard_map(
        per_device,
        mesh=torus,
        in_specs=placed,
        out_specs=(P(None, None, GX_GY_GZ), P(None, GX_GY_GZ), P(None, GX_GY_GZ)),
        check_vma=False,
    )
```

```python
import jax
import jax.numpy as jnp
from jax import lax
from jax.experimental import pallas as pl
from jax.experimental.pallas import tpu as pltpu
from jax.sharding import Mesh
from jax.sharding import PartitionSpec as P


GX = ("gx_0", "gx_1")
GZ = ("gz_0", "gz_1")
GX_GY = ("gx_0", "gx_1", "gy")
GX_GY_GZ = ("gx_0", "gx_1", "gy", "gz_0", "gz_1")
F32 = jnp.float32
PTS = 512
LANES = 128

time_step = 0.03
mass_shift = 4.0
inner_nodes = (
    -0.8717401485096066,
    -0.5917001814331423,
    -0.2092992179024789,
    0.2092992179024789,
    0.5917001814331423,
    0.8717401485096066,
)


def legendre_seven(position):
    previous = 1.0
    current_value = position
    for degree_index in range(1, 7):
        following = (
            (2 * degree_index + 1) * position * current_value - degree_index * previous
        ) / (degree_index + 1)
        previous = current_value
        current_value = following
    return current_value


def tables():
    nodes = [-1.0] + list(inner_nodes) + [1.0]
    poly = [legendre_seven(node) for node in nodes]
    weights = [2.0 / (56.0 * value * value) for value in poly]
    deriv = [[0.0] * 8 for _ in range(8)]
    for i in range(8):
        for j in range(8):
            if i != j:
                deriv[i][j] = poly[i] / (poly[j] * (nodes[i] - nodes[j]))
    deriv[0][0] = -14.0
    deriv[7][7] = 14.0
    return weights, deriv


WEIGHTS, DERIV = tables()
DERIV_T = [[DERIV[j][i] for j in range(8)] for i in range(8)]
SQUARE = [[DERIV[j][i] ** 2 for j in range(8)] for i in range(8)]
MINUS = [[-DERIV[i][j] for j in range(8)] for i in range(8)]


def mix(matrix, values, which=range(8)):
    out = []
    for i in which:
        total_value = None
        for j in range(8):
            if matrix[i][j] != 0.0:
                term = matrix[i][j] * values[j]
                total_value = term if total_value is None else total_value + term
        out.append(total_value)
    return out


def columns(matrix):
    sub = lax.broadcasted_iota(jnp.int32, (8, LANES), 0)
    out = []
    for j in range(8):
        col = jnp.zeros((8, LANES), F32)
        for i in range(8):
            col = jnp.where(sub == i, F32(matrix[i][j]), col)
        out.append(col)
    return out


def weight_column():
    sub = lax.broadcasted_iota(jnp.int32, (8, LANES), 0)
    col = jnp.zeros((8, LANES), F32)
    for i in range(8):
        col = jnp.where(sub == i, F32(WEIGHTS[i]), col)
    return col


def rows8(start):
    return pl.ds(pl.multiple_of(start, 8), 8)


def mix_inner(cols, ref, lead, start):
    total_value = None
    for j in range(8):
        term = cols[j] * ref[lead + (pl.ds(start + j, 8, stride=0), slice(None))]
        total_value = term if total_value is None else total_value + term
    return total_value


def place_of(tile):
    lane = lax.broadcasted_iota(jnp.int32, (1, LANES), 1)
    block = lane >> 4
    if tile == 0:
        row = block + 2
    else:
        row = jnp.where(block == 0, 1, jnp.where(block == 1, 10, jnp.where(block == 2, 0, 11)))
    return lane, block, lane & 15, row + 4 * (lax.axis_index("gy") - 1)


def pair_weights(has_low, has_high, average):
    own, other = (0.5, 0.5) if average else (1.0, 1.0)
    return (
        jnp.where(has_low, F32(own), F32(1.0)),
        jnp.where(has_low, F32(other), F32(0.0)),
        jnp.where(has_high, F32(own), F32(1.0)),
        jnp.where(has_high, F32(other), F32(0.0)),
    )


def x_weights(average):
    _, _, ix, _ = place_of(0)
    return pair_weights(ix > 0, ix < 15, average)


def y_weights(tile, average):
    _, _, _, y = place_of(tile)
    return pair_weights(y > 0, y < 4 * lax.axis_size("gy") - 1, average)


def z_index():
    return lax.axis_index("gz_0") * lax.axis_size("gz_1") + lax.axis_index("gz_1")


def z_weights():
    z = jnp.full((1, LANES), z_index(), jnp.int32)
    return pair_weights(z > 0, z < lax.axis_size("gz_0") * lax.axis_size("gz_1") - 1, True)


def roll(x, shift):
    return pltpu.roll(x, shift % LANES, 1)


def x_join(ref, lead, w):
    low, high = lead + (slice(0, 64),), lead + (slice(448, 512),)
    f0, f7 = ref[low], ref[high]
    ref[low] = w[0] * f0 + w[1] * roll(f7, 1)
    ref[high] = w[2] * f7 + w[3] * roll(f0, -1)


def y_join(ref, lead, w):
    for a in range(8):
        low, high = lead + (slice(64 * a, 64 * a + 8),), lead + (slice(64 * a + 56, 64 * a + 64),)
        f0, f7 = ref[low], ref[high]
        ref[low] = w[0] * f0 + w[1] * roll(f7, 16)
        ref[high] = w[2] * f7 + w[3] * roll(f0, -16)


def y_join_two(ref, far, lead, w, far_w):
    _, block, _, _ = place_of(0)
    for a in range(8):
        low, high = lead + (slice(64 * a, 64 * a + 8),), lead + (slice(64 * a + 56, 64 * a + 64),)
        f0, f7, g0, g7 = ref[low], ref[high], far[low], far[high]
        below = jnp.where(block == 0, g7, roll(f7, 16))
        above = jnp.where(block == 7, roll(g0, -32), roll(f0, -16))
        ref[low] = w[0] * f0 + w[1] * below
        ref[high] = w[2] * f7 + w[3] * above
        if far_w is not None:
            below = jnp.where(block == 0, roll(g7, -32), roll(f7, 32))
            above = jnp.where(block == 0, f0, roll(g0, -32))
            far[low] = far_w[0] * g0 + far_w[1] * below
            far[high] = far_w[2] * g7 + far_w[3] * above


def face(ref, lead, c):
    return ref[lead + (pl.ds(c, 64, stride=8), slice(None))]


def set_face(ref, lead, c, value):
    ref[lead + (pl.ds(c, 64, stride=8), slice(None))] = value


def convect(i, v, vel, out, minus_cols):
    def along_a(b, carry):
        start = 8 * b
        got = mix(MINUS, [v[i, rows8(64 * a + start)] for a in range(8)])
        for a in range(8):
            at = rows8(64 * a + start)
            out[i, at] = vel[0, at] * got[a]
        return carry

    lax.fori_loop(0, 8, along_a, 0)

    def along_bc(a, carry):
        start = 64 * a
        got = mix(MINUS, [v[i, rows8(start + 8 * b)] for b in range(8)])
        for b in range(8):
            at = rows8(start + 8 * b)
            inner = mix_inner(minus_cols, v, (i,), start + 8 * b)
            out[i, at] = out[i, at] + (vel[1, at] * got[b] + vel[2, at] * inner)
        return carry

    lax.fori_loop(0, 8, along_bc, 0)


def convect_y_faces(i, v, vel, out, minus_cols):
    for b in (0, 7):
        got = mix(MINUS, [v[i, slice(64 * a + 8 * b, 64 * a + 8 * b + 8)] for a in range(8)])
        for a in range(8):
            at = slice(64 * a + 8 * b, 64 * a + 8 * b + 8)
            out[i, at] = vel[0, at] * got[a]

    def along_bc(a, carry):
        start = 64 * a
        got = mix(MINUS, [v[i, rows8(start + 8 * b)] for b in range(8)], (0, 7))
        for b, value in zip((0, 7), got):
            at = rows8(start + 8 * b)
            inner = mix_inner(minus_cols, v, (i,), start + 8 * b)
            out[i, at] = out[i, at] + (vel[1, at] * value + vel[2, at] * inner)
        return carry

    lax.fori_loop(0, 8, along_bc, 0)


def pack_kernel(place, vel, inv, out, up, down):
    def move(s, carry):
        q = place[s]
        r = (q % 4) * 4 + q // 4
        for i in range(3):
            out[pl.ds(16 * i + r, 1), :] = vel[i, pl.ds(s, 1), :]
        out[pl.ds(48 + r, 1), :] = inv[pl.ds(s, 1), :]
        return carry

    lax.fori_loop(0, 16, move, 0)
    for ref, first in ((up, 52), (down, 48)):
        ref[0:48, :] = out[0:48, :]
        ref[48:60, :] = out[slice(first, first + 12), :]


FAR_ROWS = (1, 10, 0, 11)


def unpack(middle, sides, i, near, far, scratch, lead):
    for r in range(12):
        base = 16 * (r - 2) if 2 <= r <= 9 else LANES + 16 * FAR_ROWS.index(r)
        first = 16 * i + 4 * (r % 4)
        if r < 4 and i == 3:
            first -= 4
        if r >= 8:
            first += 60
        for g in range(4):
            at = slice(base + 4 * g, base + 4 * g + 4)
            if i == 3 and r in (0, 11):
                scratch[at, :] = jnp.zeros((4, PTS), F32)
            else:
                src = middle if 4 <= r < 8 else sides
                scratch[at, :] = src[g, slice(first, first + 4), :]
    for p in range(4):
        at = slice(128 * p, 128 * p + 128)
        near[lead + (at,)] = jnp.transpose(scratch[0:128, at])
        far[lead + (at,)] = jnp.transpose(scratch[128:256, at])


def first_kernel(middle, sides, vel, vel_far, rate, rate_far, up, down, inv, inv_far, scratch):
    scratch[192:256, :] = jnp.zeros((64, PTS), F32)
    for i in range(3):
        unpack(middle, sides, i, vel, vel_far, scratch, (i,))
    unpack(middle, sides, 3, inv, inv_far, scratch, ())
    minus_cols = columns(MINUS)
    xw = x_weights(True)
    yw = y_weights(0, True)
    fw = y_weights(1, True)

    def component(i, carry):
        convect(i, vel, vel, rate, minus_cols)
        convect(i, vel_far, vel_far, rate_far, minus_cols)
        x_join(rate, (i,), xw)
        x_join(rate_far, (i,), xw)
        y_join_two(rate, rate_far, (i,), yw, fw)
        return carry

    lax.fori_loop(0, 3, component, 0)
    lane, _, _, _ = place_of(0)
    for c, out in ((7, up), (0, down)):
        for i in range(3):
            out[slice(64 * i, 64 * i + 64), :] = face(rate, (i,), c)
        far = [face(rate_far, (i,), c) for i in range(3)]
        out[192:256, :] = jnp.where(
            lane < 32, far[0], jnp.where(lane < 64, roll(far[1], 32), roll(far[2], 64))
        )


def advance(vel, rate, below, above, acc_in, scale, acc_scale, v, acc):
    zw = z_weights()

    def step(k, carry):
        at = rows8(8 * k)
        for i in range(3):
            r = rate[i, at]
            v[i, at] = vel[i, at] + scale * r
            if acc is not None:
                acc[i, at] = acc_in[i, at] + acc_scale * r
        return carry

    lax.fori_loop(0, 64, step, 0, unroll=2)
    for i in range(3):
        for c, got, own, other in ((0, below, zw[0], zw[1]), (7, above, zw[2], zw[3])):
            k = own * face(rate, (i,), c) + other * got[i]
            set_face(v, (i,), c, face(vel, (i,), c) + scale * k)
            if acc is not None:
                set_face(acc, (i,), c, face(acc_in, (i,), c) + acc_scale * k)


def thirds(ref):
    return [ref[slice(64 * i, 64 * i + 64), :] for i in range(3)]


def second_kernel(
    vel, vel_far, rate, rate_far, below, above, acc, out, up, down, v, v_far, out_far
):
    advance(
        vel, rate, thirds(below), thirds(above), vel, 0.5 * time_step, time_step / 6.0, v, acc
    )
    far = [[roll(ref[192:256, :], -32 * i) for i in range(3)] for ref in (below, above)]
    advance(vel_far, rate_far, far[0], far[1], None, 0.5 * time_step, 0.0, v_far, None)
    minus_cols = columns(MINUS)
    xw = x_weights(True)
    yw = y_weights(0, True)

    def component(i, carry):
        convect(i, v, vel, out, minus_cols)
        convect_y_faces(i, v_far, vel_far, out_far, minus_cols)
        x_join(out, (i,), xw)
        x_join_faces(out_far, i, xw)
        y_join_two(out, out_far, (i,), yw, None)
        return carry

    lax.fori_loop(0, 3, component, 0)
    send_faces(out, up, down)


def x_join_faces(ref, i, w):
    for b in (0, 7):
        low, high = slice(8 * b, 8 * b + 8), slice(448 + 8 * b, 448 + 8 * b + 8)
        f0, f7 = ref[i, low], ref[i, high]
        ref[i, low] = w[0] * f0 + w[1] * roll(f7, 1)
        ref[i, high] = w[2] * f7 + w[3] * roll(f0, -1)


def send_faces(rate, up, down):
    for i in range(3):
        up[slice(64 * i, 64 * i + 64), :] = face(rate, (i,), 7)
        down[slice(64 * i, 64 * i + 64), :] = face(rate, (i,), 0)


def stage_kernel(scale, acc_scale):
    def kernel(vel, acc_in, rate, below, above, acc, out, up, down, v):
        advance(vel, rate, thirds(below), thirds(above), acc_in, scale, acc_scale, v, acc)
        minus_cols = columns(MINUS)
        xw = x_weights(True)
        yw = y_weights(0, True)

        def component(i, carry):
            convect(i, v, vel, out, minus_cols)
            x_join(out, (i,), xw)
            y_join(out, (i,), yw)
            return carry

        lax.fori_loop(0, 3, component, 0)
        send_faces(out, up, down)

    return kernel


def own_rows():
    _, block, _, _ = place_of(0)
    return block


def source_kernel(acc_in, rate, below, above, advected, source, up, down, joined):
    advance(acc_in, rate, thirds(below), thirds(above), None, time_step / 6.0, 0.0, advected, None)
    cols = columns(DERIV)
    wc = weight_column()

    def along_a(b, carry):
        start = 8 * b
        got = mix(DERIV, [advected[0, rows8(64 * a + start)] for a in range(8)])
        for a in range(8):
            source[rows8(64 * a + start)] = got[a]
        return carry

    lax.fori_loop(0, 8, along_a, 0)
    for a in range(8):
        start = 64 * a
        got = mix(DERIV, [advected[1, slice(start + 8 * b, start + 8 * b + 8)] for b in range(8)])
        for b in range(8):
            at = slice(start + 8 * b, start + 8 * b + 8)
            inner = mix_inner(cols, advected, (2,), start + 8 * b)
            scale = -WEIGHTS[a] * WEIGHTS[b] / time_step
            source[at] = (source[at] + got[b] + inner) * (scale * wc)
    joined[...] = source[...]
    block = own_rows()
    take_low = jnp.where((block >= 3) & (block <= 5), F32(1.0), F32(0.0))
    take_high = jnp.where((block >= 2) & (block <= 4), F32(1.0), F32(0.0))
    y_join(joined, (), (1.0, take_low, 1.0, take_high))
    lane, _, _, _ = place_of(0)
    for out, first in ((down, 1), (up, 2)):
        total_value = None
        for q in range(4):
            part = roll(joined[slice(128 * q, 128 * q + 128), :], 32 * (q - first))
            total_value = part if q == 0 else jnp.where(lane >> 5 == q, part, total_value)
        out[...] = total_value


def spread_kernel(joined, below, above, diag_up, diag_down, full, up, down):
    lane, block, _, _ = place_of(0)
    for q in range(4):
        at = slice(128 * q, 128 * q + 128)
        full[at, :] = jnp.where(
            lane < 32,
            roll(below[...], -32 * q),
            jnp.where(lane >= 96, roll(above[...], 96 - 32 * q), joined[at, :]),
        )
    take_low = jnp.where((block == 2) | (block == 6), F32(1.0), F32(0.0))
    take_high = jnp.where((block == 1) | (block == 5), F32(1.0), F32(0.0))
    y_join(full, (), (1.0, take_low, 1.0, take_high))
    x_join(full, (), x_weights(False))
    up[0:64, :] = face(full, (), 7)
    up[64:128, :] = diag_up[...]
    down[0:64, :] = face(full, (), 0)
    down[64:128, :] = diag_down[...]


def diagonal_kernel(inv, inv_far, weighted, diag, up, down, weighted_far, diag_far):
    wc = weight_column()
    cols = columns(SQUARE)
    for a in range(8):
        for b in range(8):
            at = slice(64 * a + 8 * b, 64 * a + 8 * b + 8)
            scale = WEIGHTS[a] * WEIGHTS[b] * wc
            weighted[at] = scale * inv[at]
            weighted_far[at] = scale * inv_far[at]
    for src, out, bs in ((weighted, diag, range(8)), (weighted_far, diag_far, (0, 7))):
        for b in bs:
            got = mix(SQUARE, [src[slice(64 * a + 8 * b, 64 * a + 8 * b + 8)] for a in range(8)])
            for a in range(8):
                out[slice(64 * a + 8 * b, 64 * a + 8 * b + 8)] = got[a]
        for a in range(8):
            start = 64 * a
            got = mix(SQUARE, [src[slice(start + 8 * b, start + 8 * b + 8)] for b in range(8)], bs)
            for b, value in zip(bs, got):
                at = slice(start + 8 * b, start + 8 * b + 8)
                inner = mix_inner(cols, src, (), start + 8 * b)
                scale = mass_shift * WEIGHTS[a] * WEIGHTS[b]
                out[at] = out[at] + value + inner + scale * wc
    xw = x_weights(False)
    x_join(diag, (), xw)
    for b in (0, 7):
        low, high = slice(8 * b, 8 * b + 8), slice(448 + 8 * b, 448 + 8 * b + 8)
        f0, f7 = diag_far[low], diag_far[high]
        diag_far[low] = xw[0] * f0 + xw[1] * roll(f7, 1)
        diag_far[high] = xw[2] * f7 + xw[3] * roll(f0, -1)
    y_join_two(diag, diag_far, (), y_weights(0, False), None)
    up[...] = face(diag, (), 7)
    down[...] = face(diag, (), 0)


def z_sum(src, below, above, dst):
    dst[...] = src[...]
    set_face(dst, (), 0, face(src, (), 0) + below)
    set_face(dst, (), 7, face(src, (), 7) + above)


def operate(u, weighted, out, flux):
    cols = columns(DERIV)
    cols_t = columns(DERIV_T)
    _, _, _, y = place_of(0)
    inside = (y >= 0) & (y < 4 * lax.axis_size("gy"))
    wc = jnp.where(inside, weight_column(), F32(0.0))

    def along_a(b, carry):
        start = 8 * b
        at = [rows8(64 * a + start) for a in range(8)]
        slope = mix(DERIV, [u[at[a]] for a in range(8)])
        got = mix(DERIV_T, [weighted[at[a]] * slope[a] for a in range(8)])
        for a in range(8):
            out[at[a]] = got[a]
        return carry

    lax.fori_loop(0, 8, along_a, 0)

    for a in range(8):
        start = 64 * a
        at = [slice(start + 8 * b, start + 8 * b + 8) for b in range(8)]
        values = [u[at[b]] for b in range(8)]
        weights = [weighted[at[b]] for b in range(8)]
        slope = mix(DERIV, values)
        got = mix(DERIV_T, [weights[b] * slope[b] for b in range(8)])
        for b in range(8):
            flux[at[b]] = weights[b] * mix_inner(cols, u, (), start + 8 * b)
            scale = mass_shift * WEIGHTS[a] * WEIGHTS[b]
            out[at[b]] = out[at[b]] + (got[b] + (scale * wc) * values[b])

    def along_c(k, carry):
        at = rows8(8 * k)
        out[at] = out[at] + mix_inner(cols_t, flux, (), 8 * k)
        return carry

    lax.fori_loop(0, 64, along_c, 0, unroll=4)


def own_mask():
    _, block, ix, _ = place_of(0)
    gx = lax.axis_index("gx_0") * lax.axis_size("gx_1") + lax.axis_index("gx_1")
    return jnp.where((block >= 2) & (block <= 5) & ((ix >> 2) == gx), F32(1.0), F32(0.0))


def dot(left, right):
    def step(k, carry):
        at = rows8(8 * k)
        return carry + left[at] * right[at]

    return lax.fori_loop(0, 64, step, jnp.zeros((8, LANES), F32), unroll=8)


def operator_one_kernel(
    partial, below, above, diag, source, weighted,
    residual, inverse, first, local, out, up, down, sums, flux,
):
    z_sum(partial, below[0:64, :], above[0:64, :], residual)
    z_sum(diag, below[64:128, :], above[64:128, :], inverse)
    inverse[...] = 1.0 / inverse[...]
    first[...] = residual[...] * inverse[...]
    operate(first, weighted, local, flux)
    out[...] = local[...]
    x_join(out, (), x_weights(False))
    y_join(out, (), y_weights(0, False))
    up[...] = face(out, (), 7)
    down[...] = face(out, (), 0)
    sums[0] = dot(source, first)
    sums[1] = dot(local, first)


def operator_two_kernel(
    partial, below, above, inverse, weighted, local, sums,
    applied, second, out, up, down, totals, local_two, flux,
):
    z_sum(partial, below[...], above[...], applied)
    second[...] = applied[...] * inverse[...]
    operate(second, weighted, local_two, flux)
    mask = own_mask()
    lane = lax.broadcasted_iota(jnp.int32, (1, LANES), 1)
    row = jnp.zeros((1, LANES), F32)
    for k, value in enumerate((sums[0], sums[1], dot(local, second), dot(local_two, second))):
        part = jnp.sum(mask * value, axis=0, keepdims=True)
        part = jnp.sum(part, axis=1, keepdims=True)
        row = jnp.where(lane == k, part, row)
    totals[...] = jnp.broadcast_to(row[None], totals.shape)
    out[...] = local_two[...]
    x_join(out, (), x_weights(False))
    y_join(out, (), y_weights(0, False))
    up[...] = face(out, (), 7)
    down[...] = face(out, (), 0)


def to_slots(place, ref, lead, out, k, scratch):
    for p in range(4):
        at = slice(128 * p, 128 * p + 128)
        scratch[:, at] = jnp.transpose(ref[lead + (at,)])
    gx = lax.axis_index("gx_0") * lax.axis_size("gx_1") + lax.axis_index("gx_1")
    for s in range(16):
        q = place[s]
        lane = (2 + q % 4) * 16 + 4 * gx + q // 4
        out[k, slice(s, s + 1), :] = scratch[pl.ds(lane, 1), :]


def advected_kernel(place, advected, out, scratch):
    for i in range(3):
        to_slots(place, advected, (i,), out, i, scratch)


def fields_kernel(place, left, right, out, scratch):
    to_slots(place, left, (), out, 0, scratch)
    to_slots(place, right, (), out, 1, scratch)


def last_kernel(place, partial, below, above, out, full, scratch):
    z_sum(partial, below[...], above[...], full)
    to_slots(place, full, (), out, 0, scratch)


def gather_kernel(pieces, out):
    row = jnp.sum(pieces[...], axis=0)
    out[...] = jnp.broadcast_to(row[None], out.shape)


def final_kernel(pieces, early, late, last, pressure, residual):
    row = jnp.sum(pieces[...], axis=0)
    rho, curvature, cross, tail = (row[:, k : k + 1] for k in range(4))
    step = rho / curvature
    rho_next = step * step * cross - rho
    ratio = rho_next / rho
    step_next = rho_next / (
        curvature - 2.0 * step * cross + step * step * tail - ratio * ratio * curvature
    )
    keep = step + step_next * (1.0 + ratio)
    both = step_next * step
    pressure[...] = keep * early[1] - both * late[1]
    residual[...] = early[0] - keep * late[0] + both * last[0]


def call(kernel, outs, scratch=(), scalars=0, limit=16):
    def run(*args):
        vm = pl.BlockSpec(memory_space=pltpu.VMEM)
        sm = pl.BlockSpec(memory_space=pltpu.SMEM)
        result = pl.pallas_call(
            kernel,
            out_shape=tuple(jax.ShapeDtypeStruct(shape, F32) for shape in outs),
            in_specs=[sm] * scalars + [vm] * (len(args) - scalars),
            out_specs=tuple(vm for _ in outs),
            scratch_shapes=[pltpu.VMEM(shape, F32) for shape in scratch],
            compiler_params=pltpu.CompilerParams(vmem_limit_bytes=limit * 1024 * 1024),
        )(*args)
        return result

    return run


def shift(values, axis, step):
    count = lax.axis_size(axis)
    pairs = [(i, i + step) for i in range(count) if 0 <= i + step < count]
    return lax.ppermute(values, axis, pairs)


def along(axis, up, down):
    return shift(up, axis, 1), shift(down, axis, -1)


FULL = (PTS, LANES)
THREE = (3, PTS, LANES)
FACE = (64, LANES)


def step(velocity, inv_density, element_place):
    by_slot = jnp.transpose(velocity, (0, 2, 1))
    inv_slot = jnp.transpose(inv_density)
    block, up, down = call(pack_kernel, [(64, PTS), (60, PTS), (60, PTS)], scalars=1)(
        element_place, by_slot, inv_slot
    )
    below, above = along("gy", up, down)
    middle = lax.all_gather(block, GX)
    sides = lax.all_gather(jnp.concatenate([below, above]), GX)
    vel, vel_far, rate, rate_far, up, down, inv, inv_far = call(
        first_kernel,
        [THREE, THREE, THREE, THREE, (256, LANES), (256, LANES), FULL, FULL],
        [(256, PTS)],
    )(middle, sides)
    below, above = along(GZ, up, down)
    weighted, diag, diag_up, diag_down = call(
        diagonal_kernel, [FULL, FULL, FACE, FACE], [FULL, FULL]
    )(inv, inv_far)
    acc, rate, up, down = call(
        second_kernel, [THREE, THREE, (192, LANES), (192, LANES)], [THREE, THREE, THREE]
    )(vel, vel_far, rate, rate_far, below, above)
    for scale in (0.5 * time_step, time_step):
        below, above = along(GZ, up, down)
        acc, rate, up, down = call(
            stage_kernel(scale, time_step / 3.0),
            [THREE, THREE, (192, LANES), (192, LANES)],
            [THREE],
        )(vel, acc, rate, below, above)
    below, above = along(GZ, up, down)
    advected, source, up, down, joined = call(
        source_kernel, [THREE, FULL, (128, LANES), (128, LANES), FULL]
    )(acc, rate, below, above)
    below, above = along("gy", up, down)
    (advected_slots,) = call(advected_kernel, [(3, 16, PTS)], [(LANES, PTS)], 1)(
        element_place, advected
    )
    full, up, down = call(spread_kernel, [FULL, (128, LANES), (128, LANES)])(
        joined, below, above, diag_up, diag_down
    )
    below, above = along(GZ, up, down)
    residual, inverse, first, local, partial, up, down, sums = call(
        operator_one_kernel, [FULL, FULL, FULL, FULL, FULL, FACE, FACE, (2, 8, LANES)], [FULL]
    )(full, below, above, diag, source, weighted)
    below, above = along(GZ, up, down)
    (early,) = call(fields_kernel, [(2, 16, PTS)], [(LANES, PTS)], 1)(
        element_place, residual, first
    )
    applied, second, partial, up, down, totals = call(
        operator_two_kernel, [FULL, FULL, FULL, FACE, FACE, (16, 1, LANES)], [FULL, FULL]
    )(partial, below, above, inverse, weighted, local, sums)
    below, above = along(GZ, up, down)
    pieces = lax.all_to_all(totals, GX_GY, 0, 0)
    count = lax.axis_size(GZ)
    (pieces,) = call(gather_kernel, [(count, 1, LANES)])(pieces)
    (late,) = call(fields_kernel, [(2, 16, PTS)], [(LANES, PTS)], 1)(element_place, applied, second)
    (last,) = call(last_kernel, [(1, 16, PTS)], [FULL, (LANES, PTS)], 1)(
        element_place, partial, below, above
    )
    pieces = lax.all_to_all(pieces, GZ, 0, 0)
    pressure, residual = call(final_kernel, [(16, PTS), (16, PTS)])(pieces, early, late, last)
    return (
        jnp.transpose(advected_slots, (0, 2, 1)),
        jnp.transpose(pressure),
        jnp.transpose(residual),
    )


def solution(mesh):
    torus = Mesh(
        mesh.devices.reshape(2, 2, mesh.shape["gy"], -1, 2),
        ("gx_0", "gx_1", "gy", "gz_0", "gz_1"),
    )
    placed = (P(None, None, GX_GY_GZ), P(None, GX_GY_GZ), P(GX_GY_GZ))
    return jax.shard_map(
        step,
        mesh=torus,
        in_specs=placed,
        out_specs=(P(None, None, GX_GY_GZ), P(None, GX_GY_GZ), P(None, GX_GY_GZ)),
        check_vma=False,
    )
```

```python
import jax
import jax.numpy as jnp
from jax import lax
from jax.experimental import pallas as pl
from jax.experimental.pallas import tpu as pltpu
from jax.sharding import Mesh
from jax.sharding import PartitionSpec as P


GX = ("gx_0", "gx_1")
GZ = ("gz_0", "gz_1")
PLANE = ("gx_0", "gx_1", "gy", "gz_1")
GX_GY_GZ = ("gx_0", "gx_1", "gy", "gz_0", "gz_1")
F32 = jnp.float32
PTS = 512
LANES = 128

time_step = 0.03
mass_shift = 4.0
inner_nodes = (
    -0.8717401485096066,
    -0.5917001814331423,
    -0.2092992179024789,
    0.2092992179024789,
    0.5917001814331423,
    0.8717401485096066,
)


def legendre_seven(position):
    previous = 1.0
    current_value = position
    for degree_index in range(1, 7):
        following = (
            (2 * degree_index + 1) * position * current_value - degree_index * previous
        ) / (degree_index + 1)
        previous = current_value
        current_value = following
    return current_value


def tables():
    nodes = [-1.0] + list(inner_nodes) + [1.0]
    poly = [legendre_seven(node) for node in nodes]
    weights = [2.0 / (56.0 * value * value) for value in poly]
    deriv = [[0.0] * 8 for _ in range(8)]
    for i in range(8):
        for j in range(8):
            if i != j:
                deriv[i][j] = poly[i] / (poly[j] * (nodes[i] - nodes[j]))
    deriv[0][0] = -14.0
    deriv[7][7] = 14.0
    return weights, deriv


WEIGHTS, DERIV = tables()
DERIV_T = [[DERIV[j][i] for j in range(8)] for i in range(8)]
SQUARE = [[DERIV[j][i] ** 2 for j in range(8)] for i in range(8)]
MINUS = [[-DERIV[i][j] for j in range(8)] for i in range(8)]


def mix(matrix, values, which=range(8)):
    sign = 1.0 if matrix is SQUARE else -1.0
    plus = [values[j] + values[7 - j] for j in range(4)]
    minus = [values[j] - values[7 - j] for j in range(4)]
    done = {}
    for i in sorted({min(i, 7 - i) for i in which}):
        even = odd = None
        for j in range(4):
            p, q = matrix[i][j], matrix[i][7 - j]
            e, o = 0.5 * (p + q) * plus[j], 0.5 * (p - q) * minus[j]
            even = e if even is None else even + e
            odd = o if odd is None else odd + o
        done[i] = odd + even
        done[7 - i] = even - odd if sign > 0 else odd - even
    return [done[i] for i in which]


def columns(matrix):
    sub = lax.broadcasted_iota(jnp.int32, (8, LANES), 0)
    out = []
    for j in range(8):
        col = jnp.zeros((8, LANES), F32)
        for i in range(8):
            col = jnp.where(sub == i, F32(matrix[i][j]), col)
        out.append(col)
    return out


def weight_column():
    sub = lax.broadcasted_iota(jnp.int32, (8, LANES), 0)
    col = jnp.zeros((8, LANES), F32)
    for i in range(8):
        col = jnp.where(sub == i, F32(WEIGHTS[i]), col)
    return col


def rows8(start):
    return pl.ds(pl.multiple_of(start, 8), 8)


def mix_inner(cols, ref, lead, start):
    total_value = None
    for j in range(8):
        term = cols[j] * ref[lead + (pl.ds(start + j, 8, stride=0), slice(None))]
        total_value = term if total_value is None else total_value + term
    return total_value


def place_of(tile):
    lane = lax.broadcasted_iota(jnp.int32, (1, LANES), 1)
    block = lane >> 4
    if tile == 0:
        row = block + 2
    else:
        row = jnp.where(block == 0, 1, jnp.where(block == 1, 10, jnp.where(block == 2, 0, 11)))
    return lane, block, lane & 15, row + 4 * (lax.axis_index("gy") - 1)


def pair_weights(has_low, has_high, average):
    own, other = (0.5, 0.5) if average else (1.0, 1.0)
    return (
        jnp.where(has_low, F32(own), F32(1.0)),
        jnp.where(has_low, F32(other), F32(0.0)),
        jnp.where(has_high, F32(own), F32(1.0)),
        jnp.where(has_high, F32(other), F32(0.0)),
    )


def x_weights(average):
    _, _, ix, _ = place_of(0)
    return pair_weights(ix > 0, ix < 15, average)


def y_weights(tile, average):
    _, _, _, y = place_of(tile)
    return pair_weights(y > 0, y < 4 * lax.axis_size("gy") - 1, average)


def z_index():
    return lax.axis_index("gz_0") * lax.axis_size("gz_1") + lax.axis_index("gz_1")


def z_weights():
    z = jnp.full((1, LANES), z_index(), jnp.int32)
    return pair_weights(z > 0, z < lax.axis_size("gz_0") * lax.axis_size("gz_1") - 1, True)


def roll(x, shift):
    return pltpu.roll(x, shift % LANES, 1)


def x_join(ref, lead, w):
    low, high = lead + (slice(0, 64),), lead + (slice(448, 512),)
    f0, f7 = ref[low], ref[high]
    ref[low] = w[0] * f0 + w[1] * roll(f7, 1)
    ref[high] = w[2] * f7 + w[3] * roll(f0, -1)


def y_join(ref, lead, w):
    for a in range(8):
        low, high = lead + (slice(64 * a, 64 * a + 8),), lead + (slice(64 * a + 56, 64 * a + 64),)
        f0, f7 = ref[low], ref[high]
        ref[low] = w[0] * f0 + w[1] * roll(f7, 16)
        ref[high] = w[2] * f7 + w[3] * roll(f0, -16)


def y_join_two(ref, far, lead, w, far_w):
    _, block, _, _ = place_of(0)
    for a in range(8):
        low, high = lead + (slice(64 * a, 64 * a + 8),), lead + (slice(64 * a + 56, 64 * a + 64),)
        f0, f7, g0, g7 = ref[low], ref[high], far[low], far[high]
        below = jnp.where(block == 0, g7, roll(f7, 16))
        above = jnp.where(block == 7, roll(g0, -32), roll(f0, -16))
        ref[low] = w[0] * f0 + w[1] * below
        ref[high] = w[2] * f7 + w[3] * above
        if far_w is not None:
            below = jnp.where(block == 0, roll(g7, -32), roll(f7, 32))
            above = jnp.where(block == 0, f0, roll(g0, -32))
            far[low] = far_w[0] * g0 + far_w[1] * below
            far[high] = far_w[2] * g7 + far_w[3] * above


def odd_place():
    return lax.axis_index("gz_1")


def route(near, other, at, low, high):
    odd = jnp.full((1, LANES), odd_place(), jnp.int32) == 1
    near[at, :] = jnp.where(odd, low, high)
    other[at, :] = jnp.where(odd, high, low)


def arrived(both, across, at):
    odd = jnp.full((1, LANES), odd_place(), jnp.int32) == 1
    pair, link = both[1 - odd_place(), at, :], across[at, :]
    return jnp.where(odd, pair, link), jnp.where(odd, link, pair)


def face(ref, lead, c):
    return ref[lead + (pl.ds(c, 64, stride=8), slice(None))]


def set_face(ref, lead, c, value):
    ref[lead + (pl.ds(c, 64, stride=8), slice(None))] = value


def convect(i, v, vel, out, minus_cols):
    def along_a(b, carry):
        start = 8 * b
        got = mix(MINUS, [v[i, rows8(64 * a + start)] for a in range(8)])
        for a in range(8):
            at = rows8(64 * a + start)
            out[i, at] = vel[0, at] * got[a]
        return carry

    lax.fori_loop(0, 8, along_a, 0)

    def along_bc(a, carry):
        start = 64 * a
        got = mix(MINUS, [v[i, rows8(start + 8 * b)] for b in range(8)])
        for b in range(8):
            at = rows8(start + 8 * b)
            inner = mix_inner(minus_cols, v, (i,), start + 8 * b)
            out[i, at] = out[i, at] + (vel[1, at] * got[b] + vel[2, at] * inner)
        return carry

    lax.fori_loop(0, 8, along_bc, 0)


def convect_y_faces(i, v, vel, out, minus_cols):
    for b in (0, 7):
        got = mix(MINUS, [v[i, slice(64 * a + 8 * b, 64 * a + 8 * b + 8)] for a in range(8)])
        for a in range(8):
            at = slice(64 * a + 8 * b, 64 * a + 8 * b + 8)
            out[i, at] = vel[0, at] * got[a]

    def along_bc(a, carry):
        start = 64 * a
        got = mix(MINUS, [v[i, rows8(start + 8 * b)] for b in range(8)], (0, 7))
        for b, value in zip((0, 7), got):
            at = rows8(start + 8 * b)
            inner = mix_inner(minus_cols, v, (i,), start + 8 * b)
            out[i, at] = out[i, at] + (vel[1, at] * value + vel[2, at] * inner)
        return carry

    lax.fori_loop(0, 8, along_bc, 0)


def pack_kernel(place, vel_hbm, inv_hbm, out, up, down, vel, inv, sems):
    copies = [
        pltpu.make_async_copy(vel_hbm, vel, sems.at[0]),
        pltpu.make_async_copy(inv_hbm, inv, sems.at[1]),
    ]
    for copy in copies:
        copy.start()
    for copy in copies:
        copy.wait()

    def move(s, carry):
        q = place[s]
        r = (q % 4) * 4 + q // 4
        for i in range(3):
            out[pl.ds(16 * i + r, 1), :] = vel[i, pl.ds(s, 1), :]
        out[pl.ds(48 + r, 1), :] = inv[pl.ds(s, 1), :]
        return carry

    lax.fori_loop(0, 16, move, 0)
    for ref, first in ((up, 52), (down, 48)):
        ref[0:48, :] = out[0:48, :]
        ref[48:60, :] = out[slice(first, first + 12), :]


FAR_ROWS = (1, 10, 0, 11)


def unpack(middle, sides, i, near, far, scratch, lead):
    for r in range(12):
        base = 16 * (r - 2) if 2 <= r <= 9 else LANES + 16 * FAR_ROWS.index(r)
        first = 16 * i + 4 * (r % 4)
        if r < 4 and i == 3:
            first -= 4
        if r >= 8:
            first += 60
        for g in range(4):
            at = slice(base + 4 * g, base + 4 * g + 4)
            if i == 3 and r in (0, 11):
                scratch[at, :] = jnp.zeros((4, PTS), F32)
            else:
                src = middle if 4 <= r < 8 else sides
                scratch[at, :] = src[g, slice(first, first + 4), :]
    for p in range(4):
        at = slice(128 * p, 128 * p + 128)
        near[lead + (at,)] = jnp.transpose(scratch[0:128, at])
        far[lead + (at,)] = jnp.transpose(scratch[128:256, at])


def first_kernel(middle, sides, vel, vel_far, rate, rate_far, up, down, inv, inv_far, scratch):
    scratch[192:256, :] = jnp.zeros((64, PTS), F32)
    for i in range(3):
        unpack(middle, sides, i, vel, vel_far, scratch, (i,))
    unpack(middle, sides, 3, inv, inv_far, scratch, ())
    minus_cols = columns(MINUS)
    xw = x_weights(True)
    yw = y_weights(0, True)
    fw = y_weights(1, True)

    def component(i, carry):
        convect(i, vel, vel, rate, minus_cols)
        convect(i, vel_far, vel_far, rate_far, minus_cols)
        x_join(rate, (i,), xw)
        x_join(rate_far, (i,), xw)
        y_join_two(rate, rate_far, (i,), yw, fw)
        return carry

    lax.fori_loop(0, 3, component, 0)
    lane, _, _, _ = place_of(0)
    for i in range(3):
        at = slice(64 * i, 64 * i + 64)
        route(up, down, at, face(rate, (i,), 0), face(rate, (i,), 7))
    ends = []
    for c in (0, 7):
        far = [face(rate_far, (i,), c) for i in range(3)]
        ends.append(
            jnp.where(lane < 32, far[0], jnp.where(lane < 64, roll(far[1], 32), roll(far[2], 64)))
        )
    route(up, down, slice(192, 256), *ends)


def advance(vel, rate, below, above, acc_in, scale, acc_scale, v, acc):
    zw = z_weights()

    def step(k, carry):
        at = rows8(8 * k)
        for i in range(3):
            r = rate[i, at]
            v[i, at] = vel[i, at] + scale * r
            if acc is not None:
                acc[i, at] = acc_in[i, at] + acc_scale * r
        return carry

    lax.fori_loop(0, 64, step, 0, unroll=2)
    for i in range(3):
        for c, got, own, other in ((0, below, zw[0], zw[1]), (7, above, zw[2], zw[3])):
            k = own * face(rate, (i,), c) + other * got[i]
            set_face(v, (i,), c, face(vel, (i,), c) + scale * k)
            if acc is not None:
                set_face(acc, (i,), c, face(acc_in, (i,), c) + acc_scale * k)


def thirds(both, across):
    got = [arrived(both, across, slice(64 * i, 64 * i + 64)) for i in range(3)]
    return [pair[0] for pair in got], [pair[1] for pair in got]


def second_kernel(
    vel, vel_far, rate, rate_far, below, above, acc, out, up, down, v, v_far, out_far
):
    advance(
        vel, rate, *thirds(below, above), vel, 0.5 * time_step, time_step / 6.0, v, acc
    )
    far = arrived(below, above, slice(192, 256))
    far = [[roll(part, -32 * i) for i in range(3)] for part in far]
    advance(vel_far, rate_far, far[0], far[1], None, 0.5 * time_step, 0.0, v_far, None)
    minus_cols = columns(MINUS)
    xw = x_weights(True)
    yw = y_weights(0, True)

    def component(i, carry):
        convect(i, v, vel, out, minus_cols)
        convect_y_faces(i, v_far, vel_far, out_far, minus_cols)
        x_join(out, (i,), xw)
        x_join_faces(out_far, i, xw)
        y_join_two(out, out_far, (i,), yw, None)
        return carry

    lax.fori_loop(0, 3, component, 0)
    send_faces(out, up, down)


def x_join_faces(ref, i, w):
    for b in (0, 7):
        low, high = slice(8 * b, 8 * b + 8), slice(448 + 8 * b, 448 + 8 * b + 8)
        f0, f7 = ref[i, low], ref[i, high]
        ref[i, low] = w[0] * f0 + w[1] * roll(f7, 1)
        ref[i, high] = w[2] * f7 + w[3] * roll(f0, -1)


def send_faces(rate, near, other):
    for i in range(3):
        at = slice(64 * i, 64 * i + 64)
        route(near, other, at, face(rate, (i,), 0), face(rate, (i,), 7))


def stage_kernel(scale, acc_scale):
    def kernel(vel, acc_in, rate, below, above, acc, out, up, down, v):
        advance(vel, rate, *thirds(below, above), acc_in, scale, acc_scale, v, acc)
        minus_cols = columns(MINUS)
        xw = x_weights(True)
        yw = y_weights(0, True)

        def component(i, carry):
            convect(i, v, vel, out, minus_cols)
            x_join(out, (i,), xw)
            y_join(out, (i,), yw)
            return carry

        lax.fori_loop(0, 3, component, 0)
        send_faces(out, up, down)

    return kernel


def own_rows():
    _, block, _, _ = place_of(0)
    return block


def source_kernel(acc_in, rate, below, above, advected, source, up, down, joined):
    advance(acc_in, rate, *thirds(below, above), None, time_step / 6.0, 0.0, advected, None)
    cols = columns(DERIV)
    wc = weight_column()

    def along_a(b, carry):
        start = 8 * b
        got = mix(DERIV, [advected[0, rows8(64 * a + start)] for a in range(8)])
        for a in range(8):
            source[rows8(64 * a + start)] = got[a]
        return carry

    lax.fori_loop(0, 8, along_a, 0)
    for a in range(8):
        start = 64 * a
        got = mix(DERIV, [advected[1, slice(start + 8 * b, start + 8 * b + 8)] for b in range(8)])
        for b in range(8):
            at = slice(start + 8 * b, start + 8 * b + 8)
            inner = mix_inner(cols, advected, (2,), start + 8 * b)
            scale = -WEIGHTS[a] * WEIGHTS[b] / time_step
            source[at] = (source[at] + got[b] + inner) * (scale * wc)
    joined[...] = source[...]
    block = own_rows()
    take_low = jnp.where((block >= 3) & (block <= 5), F32(1.0), F32(0.0))
    take_high = jnp.where((block >= 2) & (block <= 4), F32(1.0), F32(0.0))
    y_join(joined, (), (1.0, take_low, 1.0, take_high))
    lane, _, _, _ = place_of(0)
    for out, first in ((down, 1), (up, 2)):
        total_value = None
        for q in range(4):
            part = roll(joined[slice(128 * q, 128 * q + 128), :], 32 * (q - first))
            total_value = part if q == 0 else jnp.where(lane >> 5 == q, part, total_value)
        out[...] = total_value


def spread_kernel(joined, below, above, diag_up, diag_down, full, up, down):
    lane, block, _, _ = place_of(0)
    for q in range(4):
        at = slice(128 * q, 128 * q + 128)
        full[at, :] = jnp.where(
            lane < 32,
            roll(below[...], -32 * q),
            jnp.where(lane >= 96, roll(above[...], 96 - 32 * q), joined[at, :]),
        )
    take_low = jnp.where((block == 2) | (block == 6), F32(1.0), F32(0.0))
    take_high = jnp.where((block == 1) | (block == 5), F32(1.0), F32(0.0))
    y_join(full, (), (1.0, take_low, 1.0, take_high))
    x_join(full, (), x_weights(False))
    route(up, down, slice(0, 64), face(full, (), 0), face(full, (), 7))
    route(up, down, slice(64, 128), diag_down[...], diag_up[...])


def diagonal_kernel(inv, inv_far, weighted, diag, up, down, weighted_far, diag_far):
    wc = weight_column()
    cols = columns(SQUARE)
    for a in range(8):
        for b in range(8):
            at = slice(64 * a + 8 * b, 64 * a + 8 * b + 8)
            scale = WEIGHTS[a] * WEIGHTS[b] * wc
            weighted[at] = scale * inv[at]
            weighted_far[at] = scale * inv_far[at]
    for src, out, bs in ((weighted, diag, range(8)), (weighted_far, diag_far, (0, 7))):
        for b in bs:
            got = mix(SQUARE, [src[slice(64 * a + 8 * b, 64 * a + 8 * b + 8)] for a in range(8)])
            for a in range(8):
                out[slice(64 * a + 8 * b, 64 * a + 8 * b + 8)] = got[a]
        for a in range(8):
            start = 64 * a
            got = mix(SQUARE, [src[slice(start + 8 * b, start + 8 * b + 8)] for b in range(8)], bs)
            for b, value in zip(bs, got):
                at = slice(start + 8 * b, start + 8 * b + 8)
                inner = mix_inner(cols, src, (), start + 8 * b)
                scale = mass_shift * WEIGHTS[a] * WEIGHTS[b]
                out[at] = out[at] + value + inner + scale * wc
    xw = x_weights(False)
    x_join(diag, (), xw)
    for b in (0, 7):
        low, high = slice(8 * b, 8 * b + 8), slice(448 + 8 * b, 448 + 8 * b + 8)
        f0, f7 = diag_far[low], diag_far[high]
        diag_far[low] = xw[0] * f0 + xw[1] * roll(f7, 1)
        diag_far[high] = xw[2] * f7 + xw[3] * roll(f0, -1)
    y_join_two(diag, diag_far, (), y_weights(0, False), None)
    up[...] = face(diag, (), 7)
    down[...] = face(diag, (), 0)


def z_sum(src, below, above, dst):
    dst[...] = src[...]
    set_face(dst, (), 0, face(src, (), 0) + below)
    set_face(dst, (), 7, face(src, (), 7) + above)


def operate(u, weighted, out, flux):
    cols = columns(DERIV)
    cols_t = columns(DERIV_T)
    _, _, _, y = place_of(0)
    inside = (y >= 0) & (y < 4 * lax.axis_size("gy"))
    wc = jnp.where(inside, weight_column(), F32(0.0))

    def along_a(b, carry):
        start = 8 * b
        at = [rows8(64 * a + start) for a in range(8)]
        slope = mix(DERIV, [u[at[a]] for a in range(8)])
        got = mix(DERIV_T, [weighted[at[a]] * slope[a] for a in range(8)])
        for a in range(8):
            out[at[a]] = got[a]
        return carry

    lax.fori_loop(0, 8, along_a, 0)

    for a in range(8):
        start = 64 * a
        at = [slice(start + 8 * b, start + 8 * b + 8) for b in range(8)]
        values = [u[at[b]] for b in range(8)]
        weights = [weighted[at[b]] for b in range(8)]
        slope = mix(DERIV, values)
        got = mix(DERIV_T, [weights[b] * slope[b] for b in range(8)])
        for b in range(8):
            flux[at[b]] = weights[b] * mix_inner(cols, u, (), start + 8 * b)
            scale = mass_shift * WEIGHTS[a] * WEIGHTS[b]
            out[at[b]] = out[at[b]] + (got[b] + (scale * wc) * values[b])

    def along_c(k, carry):
        at = rows8(8 * k)
        out[at] = out[at] + mix_inner(cols_t, flux, (), 8 * k)
        return carry

    lax.fori_loop(0, 64, along_c, 0, unroll=4)


def own_mask():
    _, block, ix, _ = place_of(0)
    gx = lax.axis_index("gx_0") * lax.axis_size("gx_1") + lax.axis_index("gx_1")
    return jnp.where((block >= 2) & (block <= 5) & ((ix >> 2) == gx), F32(1.0), F32(0.0))


def dot(left, right):
    def step(k, carry):
        at = rows8(8 * k)
        return carry + left[at] * right[at]

    return lax.fori_loop(0, 64, step, jnp.zeros((8, LANES), F32), unroll=8)


def operator_one_kernel(
    partial, below, above, diag, source, weighted,
    residual, inverse, first, local, out, up, down, sums, flux,
):
    zw = z_weights()
    for src, dst, first_row in ((partial, residual, 0), (diag, inverse, 64)):
        low, high = arrived(below, above, slice(first_row, first_row + 64))
        z_sum(src, jnp.where(zw[1] > 0, low, F32(0.0)), jnp.where(zw[3] > 0, high, F32(0.0)), dst)
    inverse[...] = 1.0 / inverse[...]
    first[...] = residual[...] * inverse[...]
    operate(first, weighted, local, flux)
    out[...] = local[...]
    x_join(out, (), x_weights(False))
    y_join(out, (), y_weights(0, False))
    up[...] = face(out, (), 7)
    down[...] = face(out, (), 0)
    sums[0] = dot(source, first)
    sums[1] = dot(local, first)


def operator_two_kernel(
    partial, below, above, inverse, weighted, local, sums,
    applied, second, out, up, down, totals, local_two, flux,
):
    z_sum(partial, below[...], above[...], applied)
    second[...] = applied[...] * inverse[...]
    operate(second, weighted, local_two, flux)
    mask = own_mask()
    lane = lax.broadcasted_iota(jnp.int32, (1, LANES), 1)
    row = jnp.zeros((1, LANES), F32)
    for k, value in enumerate((sums[0], sums[1], dot(local, second), dot(local_two, second))):
        part = jnp.sum(mask * value, axis=0, keepdims=True)
        part = jnp.sum(part, axis=1, keepdims=True)
        row = jnp.where(lane == k, part, row)
    totals[...] = jnp.broadcast_to(row[None], totals.shape)
    out[...] = local_two[...]
    x_join(out, (), x_weights(False))
    y_join(out, (), y_weights(0, False))
    up[...] = face(out, (), 7)
    down[...] = face(out, (), 0)


def to_slots(place, ref, lead, out, k, scratch):
    for p in range(4):
        at = slice(128 * p, 128 * p + 128)
        scratch[:, at] = jnp.transpose(ref[lead + (at,)])
    gx = lax.axis_index("gx_0") * lax.axis_size("gx_1") + lax.axis_index("gx_1")
    for s in range(16):
        q = place[s]
        lane = (2 + q % 4) * 16 + 4 * gx + q // 4
        out[k, slice(s, s + 1), :] = scratch[pl.ds(lane, 1), :]


def advected_kernel(place, advected, out, scratch):
    for i in range(3):
        to_slots(place, advected, (i,), out, i, scratch)


def fields_kernel(place, left, right, out, scratch):
    to_slots(place, left, (), out, 0, scratch)
    to_slots(place, right, (), out, 1, scratch)


def last_kernel(place, partial, below, above, out, full, scratch):
    z_sum(partial, below[...], above[...], full)
    to_slots(place, full, (), out, 0, scratch)


def gather_kernel(pieces, out):
    row = jnp.sum(pieces[...], axis=0)
    out[...] = jnp.broadcast_to(row[None], out.shape)


def final_kernel(pieces, early, late, last, pressure, residual):
    row = jnp.sum(pieces[...], axis=0)
    rho, curvature, cross, tail = (row[:, k : k + 1] for k in range(4))
    step = rho / curvature
    rho_next = step * step * cross - rho
    ratio = rho_next / rho
    step_next = rho_next / (
        curvature - 2.0 * step * cross + step * step * tail - ratio * ratio * curvature
    )
    keep = step + step_next * (1.0 + ratio)
    both = step_next * step
    pressure[...] = keep * early[1] - both * late[1]
    residual[...] = early[0] - keep * late[0] + both * last[0]


def call(kernel, outs, scratch=(), scalars=0, raw=0):
    def run(*args):
        vm = pl.BlockSpec(memory_space=pltpu.VMEM)
        sm = pl.BlockSpec(memory_space=pltpu.SMEM)
        hbm = pl.BlockSpec(memory_space=pltpu.MemorySpace.HBM)
        return pl.pallas_call(
            kernel,
            out_shape=tuple(jax.ShapeDtypeStruct(shape, F32) for shape in outs),
            in_specs=[sm] * scalars + [hbm] * raw + [vm] * (len(args) - scalars - raw),
            out_specs=tuple(vm for _ in outs),
            scratch_shapes=[pltpu.VMEM(shape, F32) for shape in scratch]
            + ([pltpu.SemaphoreType.DMA((raw,))] if raw else []),
            compiler_params=pltpu.CompilerParams(vmem_limit_bytes=16 * 1024 * 1024),
        )(*args)

    return run


def shift(values, axis, step):
    count = lax.axis_size(axis)
    pairs = [(i, i + step) for i in range(count) if 0 <= i + step < count]
    return lax.ppermute(values, axis, pairs)


def paired(near, other):
    count = lax.axis_size(GZ)
    links = [pair for i in range(1, count - 1, 2) for pair in ((i, i + 1), (i + 1, i))]
    across = lax.ppermute(other, GZ, links)
    both = lax.all_gather(near, "gz_1")
    return both, across


def along(axis, up, down):
    return shift(up, axis, 1), shift(down, axis, -1)


FULL = (PTS, LANES)
THREE = (3, PTS, LANES)
FACE = (64, LANES)


def step(velocity, inv_density, element_place):
    by_slot = jnp.transpose(velocity, (0, 2, 1))
    inv_slot = jnp.transpose(inv_density)
    block, up, down = call(
        pack_kernel, [(64, PTS), (60, PTS), (60, PTS)], [(3, 16, PTS), (16, PTS)], 1, 2
    )(element_place, by_slot, inv_slot)
    below, above = along("gy", up, down)
    middle = lax.all_gather(block, GX)
    sides = lax.all_gather(jnp.concatenate([below, above]), GX)
    vel, vel_far, rate, rate_far, up, down, inv, inv_far = call(
        first_kernel,
        [THREE, THREE, THREE, THREE, (256, LANES), (256, LANES), FULL, FULL],
        [(256, PTS)],
    )(middle, sides)
    below, above = paired(up, down)
    weighted, diag, diag_up, diag_down = call(
        diagonal_kernel, [FULL, FULL, FACE, FACE], [FULL, FULL]
    )(inv, inv_far)
    acc, rate, up, down = call(
        second_kernel, [THREE, THREE, (192, LANES), (192, LANES)], [THREE, THREE, THREE]
    )(vel, vel_far, rate, rate_far, below, above)
    for scale in (0.5 * time_step, time_step):
        below, above = paired(up, down)
        acc, rate, up, down = call(
            stage_kernel(scale, time_step / 3.0),
            [THREE, THREE, (192, LANES), (192, LANES)],
            [THREE],
        )(vel, acc, rate, below, above)
    below, above = paired(up, down)
    advected, source, up, down, joined = call(
        source_kernel, [THREE, FULL, (128, LANES), (128, LANES), FULL]
    )(acc, rate, below, above)
    below, above = along("gy", up, down)
    (advected_slots,) = call(advected_kernel, [(3, 16, PTS)], [(LANES, PTS)], 1)(
        element_place, advected
    )
    full, up, down = call(spread_kernel, [FULL, (128, LANES), (128, LANES)])(
        joined, below, above, diag_up, diag_down
    )
    below, above = paired(up, down)
    residual, inverse, first, local, partial, up, down, sums = call(
        operator_one_kernel, [FULL, FULL, FULL, FULL, FULL, FACE, FACE, (2, 8, LANES)], [FULL]
    )(full, below, above, diag, source, weighted)
    below, above = along(GZ, up, down)
    (early,) = call(fields_kernel, [(2, 16, PTS)], [(LANES, PTS)], 1)(
        element_place, residual, first
    )
    applied, second, partial, up, down, totals = call(
        operator_two_kernel, [FULL, FULL, FULL, FACE, FACE, (lax.axis_size(PLANE), 1, LANES)], [FULL, FULL]
    )(partial, below, above, inverse, weighted, local, sums)
    below, above = along(GZ, up, down)
    pieces = lax.all_to_all(totals, PLANE, 0, 0)
    count = lax.axis_size("gz_0")
    (pieces,) = call(gather_kernel, [(count, 1, LANES)])(pieces)
    (late,) = call(fields_kernel, [(2, 16, PTS)], [(LANES, PTS)], 1)(element_place, applied, second)
    (last,) = call(last_kernel, [(1, 16, PTS)], [FULL, (LANES, PTS)], 1)(
        element_place, partial, below, above
    )
    pieces = lax.all_to_all(pieces, "gz_0", 0, 0)
    pressure, residual = call(final_kernel, [(16, PTS), (16, PTS)])(pieces, early, late, last)
    return (
        jnp.transpose(advected_slots, (0, 2, 1)),
        jnp.transpose(pressure),
        jnp.transpose(residual),
    )


def solution(mesh):
    torus = Mesh(
        mesh.devices.reshape(2, 2, mesh.shape["gy"], -1, 2),
        ("gx_0", "gx_1", "gy", "gz_0", "gz_1"),
    )
    placed = (P(None, None, GX_GY_GZ), P(None, GX_GY_GZ), P(GX_GY_GZ))
    return jax.shard_map(
        step,
        mesh=torus,
        in_specs=placed,
        out_specs=(P(None, None, GX_GY_GZ), P(None, GX_GY_GZ), P(None, GX_GY_GZ)),
        check_vma=False,
    )
```

```python
import jax
import jax.numpy as jnp
from jax import lax
from jax.experimental import pallas as pl
from jax.experimental.pallas import tpu as pltpu
from jax.sharding import Mesh
from jax.sharding import PartitionSpec as P


GX = ("gx_0", "gx_1")
GZ = ("gz_0", "gz_1")
PLANE = ("gx_0", "gx_1", "gy", "gz_1")
GX_GY_GZ = ("gx_0", "gx_1", "gy", "gz_0", "gz_1")
F32 = jnp.float32
PTS = 512
LANES = 128

time_step = 0.03
mass_shift = 4.0
inner_nodes = (
    -0.8717401485096066,
    -0.5917001814331423,
    -0.2092992179024789,
    0.2092992179024789,
    0.5917001814331423,
    0.8717401485096066,
)


def legendre_seven(position):
    previous = 1.0
    current_value = position
    for degree_index in range(1, 7):
        following = (
            (2 * degree_index + 1) * position * current_value - degree_index * previous
        ) / (degree_index + 1)
        previous = current_value
        current_value = following
    return current_value


def tables():
    nodes = [-1.0] + list(inner_nodes) + [1.0]
    poly = [legendre_seven(node) for node in nodes]
    weights = [2.0 / (56.0 * value * value) for value in poly]
    deriv = [[0.0] * 8 for _ in range(8)]
    for i in range(8):
        for j in range(8):
            if i != j:
                deriv[i][j] = poly[i] / (poly[j] * (nodes[i] - nodes[j]))
    deriv[0][0] = -14.0
    deriv[7][7] = 14.0
    return weights, deriv


WEIGHTS, DERIV = tables()
DERIV_T = [[DERIV[j][i] for j in range(8)] for i in range(8)]
SQUARE = [[DERIV[j][i] ** 2 for j in range(8)] for i in range(8)]
MINUS = [[-DERIV[i][j] for j in range(8)] for i in range(8)]


def mix(matrix, values, which=range(8)):
    sign = 1.0 if matrix is SQUARE else -1.0
    plus = [values[j] + values[7 - j] for j in range(4)]
    minus = [values[j] - values[7 - j] for j in range(4)]
    done = {}
    for i in sorted({min(i, 7 - i) for i in which}):
        even = odd = None
        for j in range(4):
            p, q = matrix[i][j], matrix[i][7 - j]
            e, o = 0.5 * (p + q) * plus[j], 0.5 * (p - q) * minus[j]
            even = e if even is None else even + e
            odd = o if odd is None else odd + o
        done[i] = odd + even
        done[7 - i] = even - odd if sign > 0 else odd - even
    return [done[i] for i in which]


def columns(matrix):
    sub = lax.broadcasted_iota(jnp.int32, (8, LANES), 0)
    out = []
    for j in range(8):
        col = jnp.zeros((8, LANES), F32)
        for i in range(8):
            col = jnp.where(sub == i, F32(matrix[i][j]), col)
        out.append(col)
    return out


def weight_column():
    sub = lax.broadcasted_iota(jnp.int32, (8, LANES), 0)
    col = jnp.zeros((8, LANES), F32)
    for i in range(8):
        col = jnp.where(sub == i, F32(WEIGHTS[i]), col)
    return col


def rows8(start):
    return pl.ds(pl.multiple_of(start, 8), 8)


def mix_inner(cols, ref, lead, start):
    total_value = None
    for j in range(8):
        term = cols[j] * ref[lead + (pl.ds(start + j, 8, stride=0), slice(None))]
        total_value = term if total_value is None else total_value + term
    return total_value


def place_of(tile):
    lane = lax.broadcasted_iota(jnp.int32, (1, LANES), 1)
    block = lane >> 4
    if tile == 0:
        row = block + 2
    else:
        row = jnp.where(block == 0, 1, jnp.where(block == 1, 10, jnp.where(block == 2, 0, 11)))
    return lane, block, lane & 15, row + 4 * (lax.axis_index("gy") - 1)


def pair_weights(has_low, has_high, average):
    own, other = (0.5, 0.5) if average else (1.0, 1.0)
    return (
        jnp.where(has_low, F32(own), F32(1.0)),
        jnp.where(has_low, F32(other), F32(0.0)),
        jnp.where(has_high, F32(own), F32(1.0)),
        jnp.where(has_high, F32(other), F32(0.0)),
    )


def x_weights(average):
    _, _, ix, _ = place_of(0)
    return pair_weights(ix > 0, ix < 15, average)


def y_weights(tile, average):
    _, _, _, y = place_of(tile)
    return pair_weights(y > 0, y < 4 * lax.axis_size("gy") - 1, average)


def z_index():
    return lax.axis_index("gz_0") * lax.axis_size("gz_1") + lax.axis_index("gz_1")


def z_weights():
    z = jnp.full((1, LANES), z_index(), jnp.int32)
    return pair_weights(z > 0, z < lax.axis_size("gz_0") * lax.axis_size("gz_1") - 1, True)


def roll(x, shift):
    return pltpu.roll(x, shift % LANES, 1)


def x_join(ref, lead, w):
    low, high = lead + (slice(0, 64),), lead + (slice(448, 512),)
    f0, f7 = ref[low], ref[high]
    ref[low] = w[0] * f0 + w[1] * roll(f7, 1)
    ref[high] = w[2] * f7 + w[3] * roll(f0, -1)


def y_join(ref, lead, w):
    for a in range(8):
        low, high = lead + (slice(64 * a, 64 * a + 8),), lead + (slice(64 * a + 56, 64 * a + 64),)
        f0, f7 = ref[low], ref[high]
        ref[low] = w[0] * f0 + w[1] * roll(f7, 16)
        ref[high] = w[2] * f7 + w[3] * roll(f0, -16)


def y_join_two(ref, far, lead, w, far_w):
    _, block, _, _ = place_of(0)
    for a in range(8):
        low, high = lead + (slice(64 * a, 64 * a + 8),), lead + (slice(64 * a + 56, 64 * a + 64),)
        f0, f7, g0, g7 = ref[low], ref[high], far[low], far[high]
        below = jnp.where(block == 0, g7, roll(f7, 16))
        above = jnp.where(block == 7, roll(g0, -32), roll(f0, -16))
        ref[low] = w[0] * f0 + w[1] * below
        ref[high] = w[2] * f7 + w[3] * above
        if far_w is not None:
            below = jnp.where(block == 0, roll(g7, -32), roll(f7, 32))
            above = jnp.where(block == 0, f0, roll(g0, -32))
            far[low] = far_w[0] * g0 + far_w[1] * below
            far[high] = far_w[2] * g7 + far_w[3] * above


def odd_place():
    return lax.axis_index("gz_1")


def route(near, other, at, low, high):
    odd = jnp.full((1, LANES), odd_place(), jnp.int32) == 1
    near[at, :] = jnp.where(odd, low, high)
    other[at, :] = jnp.where(odd, high, low)


def arrived(both, across, at):
    odd = jnp.full((1, LANES), odd_place(), jnp.int32) == 1
    pair, link = both[1 - odd_place(), at, :], across[at, :]
    return jnp.where(odd, pair, link), jnp.where(odd, link, pair)


def face(ref, lead, c):
    return ref[lead + (pl.ds(c, 64, stride=8), slice(None))]


def set_face(ref, lead, c, value):
    ref[lead + (pl.ds(c, 64, stride=8), slice(None))] = value


def convect(i, v, vel, out, minus_cols):
    def along_a(b, carry):
        start = 8 * b
        got = mix(MINUS, [v[i, rows8(64 * a + start)] for a in range(8)])
        for a in range(8):
            at = rows8(64 * a + start)
            out[i, at] = vel[0, at] * got[a]
        return carry

    lax.fori_loop(0, 8, along_a, 0)

    def along_bc(a, carry):
        start = 64 * a
        got = mix(MINUS, [v[i, rows8(start + 8 * b)] for b in range(8)])
        for b in range(8):
            at = rows8(start + 8 * b)
            inner = mix_inner(minus_cols, v, (i,), start + 8 * b)
            out[i, at] = out[i, at] + (vel[1, at] * got[b] + vel[2, at] * inner)
        return carry

    lax.fori_loop(0, 8, along_bc, 0)


def convect_y_faces(i, v, vel, out, minus_cols):
    for b in (0, 7):
        got = mix(MINUS, [v[i, slice(64 * a + 8 * b, 64 * a + 8 * b + 8)] for a in range(8)])
        for a in range(8):
            at = slice(64 * a + 8 * b, 64 * a + 8 * b + 8)
            out[i, at] = vel[0, at] * got[a]

    def along_bc(a, carry):
        start = 64 * a
        got = mix(MINUS, [v[i, rows8(start + 8 * b)] for b in range(8)], (0, 7))
        for b, value in zip((0, 7), got):
            at = rows8(start + 8 * b)
            inner = mix_inner(minus_cols, v, (i,), start + 8 * b)
            out[i, at] = out[i, at] + (vel[1, at] * value + vel[2, at] * inner)
        return carry

    lax.fori_loop(0, 8, along_bc, 0)


def pack_kernel(place, vel_hbm, inv_hbm, out, up, down, vel, inv, sems):
    copies = [
        pltpu.make_async_copy(vel_hbm, vel, sems.at[0]),
        pltpu.make_async_copy(inv_hbm, inv, sems.at[1]),
    ]
    for copy in copies:
        copy.start()
    for copy in copies:
        copy.wait()

    def move(s, carry):
        q = place[s]
        r = (q % 4) * 4 + q // 4
        for i in range(3):
            out[pl.ds(16 * i + r, 1), :] = vel[i, pl.ds(s, 1), :]
        out[pl.ds(48 + r, 1), :] = inv[pl.ds(s, 1), :]
        return carry

    lax.fori_loop(0, 16, move, 0)
    for ref, first in ((up, 52), (down, 48)):
        ref[0:48, :] = out[0:48, :]
        ref[48:60, :] = out[slice(first, first + 12), :]


FAR_ROWS = (1, 10, 0, 11)


def unpack(middle, sides, i, near, far, scratch, lead):
    for r in range(12):
        base = 16 * (r - 2) if 2 <= r <= 9 else LANES + 16 * FAR_ROWS.index(r)
        first = 16 * i + 4 * (r % 4)
        if r < 4 and i == 3:
            first -= 4
        if r >= 8:
            first += 60
        for g in range(4):
            at = slice(base + 4 * g, base + 4 * g + 4)
            if i == 3 and r in (0, 11):
                scratch[at, :] = jnp.zeros((4, PTS), F32)
            else:
                src = middle if 4 <= r < 8 else sides
                scratch[at, :] = src[g, slice(first, first + 4), :]
    for p in range(4):
        at = slice(128 * p, 128 * p + 128)
        near[lead + (at,)] = jnp.transpose(scratch[0:128, at])
        far[lead + (at,)] = jnp.transpose(scratch[128:256, at])


def first_kernel(middle, sides, vel, vel_far, rate, rate_far, up, down, inv, inv_far, scratch):
    scratch[192:256, :] = jnp.zeros((64, PTS), F32)
    for i in range(3):
        unpack(middle, sides, i, vel, vel_far, scratch, (i,))
    unpack(middle, sides, 3, inv, inv_far, scratch, ())
    minus_cols = columns(MINUS)
    xw = x_weights(True)
    yw = y_weights(0, True)
    fw = y_weights(1, True)

    def component(i, carry):
        convect(i, vel, vel, rate, minus_cols)
        convect(i, vel_far, vel_far, rate_far, minus_cols)
        x_join(rate, (i,), xw)
        x_join(rate_far, (i,), xw)
        y_join_two(rate, rate_far, (i,), yw, fw)
        return carry

    lax.fori_loop(0, 3, component, 0)
    lane, _, _, _ = place_of(0)
    for i in range(3):
        at = slice(64 * i, 64 * i + 64)
        route(up, down, at, face(rate, (i,), 0), face(rate, (i,), 7))
    ends = []
    for c in (0, 7):
        far = [face(rate_far, (i,), c) for i in range(3)]
        ends.append(
            jnp.where(lane < 32, far[0], jnp.where(lane < 64, roll(far[1], 32), roll(far[2], 64)))
        )
    route(up, down, slice(192, 256), *ends)


def advance(vel, rate, below, above, acc_in, scale, acc_scale, v, acc):
    zw = z_weights()

    def step(k, carry):
        at = rows8(8 * k)
        for i in range(3):
            r = rate[i, at]
            v[i, at] = vel[i, at] + scale * r
            if acc is not None:
                acc[i, at] = acc_in[i, at] + acc_scale * r
        return carry

    lax.fori_loop(0, 64, step, 0, unroll=2)
    for i in range(3):
        for c, got, own, other in ((0, below, zw[0], zw[1]), (7, above, zw[2], zw[3])):
            k = own * face(rate, (i,), c) + other * got[i]
            set_face(v, (i,), c, face(vel, (i,), c) + scale * k)
            if acc is not None:
                set_face(acc, (i,), c, face(acc_in, (i,), c) + acc_scale * k)


def thirds(both, across):
    got = [arrived(both, across, slice(64 * i, 64 * i + 64)) for i in range(3)]
    return [pair[0] for pair in got], [pair[1] for pair in got]


def second_kernel(
    vel, vel_far, rate, rate_far, below, above, acc, out, up, down, v, v_far, out_far
):
    advance(
        vel, rate, *thirds(below, above), vel, 0.5 * time_step, time_step / 6.0, v, acc
    )
    far = arrived(below, above, slice(192, 256))
    far = [[roll(part, -32 * i) for i in range(3)] for part in far]
    advance(vel_far, rate_far, far[0], far[1], None, 0.5 * time_step, 0.0, v_far, None)
    minus_cols = columns(MINUS)
    xw = x_weights(True)
    yw = y_weights(0, True)

    def component(i, carry):
        convect(i, v, vel, out, minus_cols)
        convect_y_faces(i, v_far, vel_far, out_far, minus_cols)
        x_join(out, (i,), xw)
        x_join_faces(out_far, i, xw)
        y_join_two(out, out_far, (i,), yw, None)
        return carry

    lax.fori_loop(0, 3, component, 0)
    send_faces(out, up, down)


def x_join_faces(ref, i, w):
    for b in (0, 7):
        low, high = slice(8 * b, 8 * b + 8), slice(448 + 8 * b, 448 + 8 * b + 8)
        f0, f7 = ref[i, low], ref[i, high]
        ref[i, low] = w[0] * f0 + w[1] * roll(f7, 1)
        ref[i, high] = w[2] * f7 + w[3] * roll(f0, -1)


def send_faces(rate, near, other):
    for i in range(3):
        at = slice(64 * i, 64 * i + 64)
        route(near, other, at, face(rate, (i,), 0), face(rate, (i,), 7))


def send_own_faces(rate, near, other):
    lane, _, _, _ = place_of(0)
    ends = []
    for c in (0, 7):
        f = [face(rate, (i,), c) for i in range(3)]
        ends.append(
            (
                jnp.where(lane < 64, roll(f[0], -32), roll(f[1], 32)),
                jnp.where(lane < 64, roll(f[2][0:32], -32), roll(f[2][32:64], 32)),
            )
        )
    route(near, other, slice(0, 64), ends[0][0], ends[1][0])
    route(near, other, slice(64, 96), ends[0][1], ends[1][1])


def own_thirds(both, across):
    wide = arrived(both, across, slice(0, 64))
    rest = arrived(both, across, slice(64, 96))
    return [
        [
            roll(w, 32),
            roll(w, -32),
            jnp.concatenate([roll(r, 32), roll(r, -32)], axis=0),
        ]
        for w, r in zip(wide, rest)
    ]


def stage_kernel(scale, acc_scale, send):
    def kernel(vel, acc_in, rate, below, above, acc, out, up, down, v):
        advance(vel, rate, *thirds(below, above), acc_in, scale, acc_scale, v, acc)
        minus_cols = columns(MINUS)
        xw = x_weights(True)
        yw = y_weights(0, True)

        def component(i, carry):
            convect(i, v, vel, out, minus_cols)
            x_join(out, (i,), xw)
            y_join(out, (i,), yw)
            return carry

        lax.fori_loop(0, 3, component, 0)
        send(out, up, down)

    return kernel


def own_rows():
    _, block, _, _ = place_of(0)
    return block


def source_kernel(acc_in, rate, below, above, advected, source, up, down, joined):
    advance(acc_in, rate, *own_thirds(below, above), None, time_step / 6.0, 0.0, advected, None)
    cols = columns(DERIV)
    wc = weight_column()

    def along_a(b, carry):
        start = 8 * b
        got = mix(DERIV, [advected[0, rows8(64 * a + start)] for a in range(8)])
        for a in range(8):
            source[rows8(64 * a + start)] = got[a]
        return carry

    lax.fori_loop(0, 8, along_a, 0)
    for a in range(8):
        start = 64 * a
        got = mix(DERIV, [advected[1, slice(start + 8 * b, start + 8 * b + 8)] for b in range(8)])
        for b in range(8):
            at = slice(start + 8 * b, start + 8 * b + 8)
            inner = mix_inner(cols, advected, (2,), start + 8 * b)
            scale = -WEIGHTS[a] * WEIGHTS[b] / time_step
            source[at] = (source[at] + got[b] + inner) * (scale * wc)
    joined[...] = source[...]
    block = own_rows()
    take_low = jnp.where((block >= 3) & (block <= 5), F32(1.0), F32(0.0))
    take_high = jnp.where((block >= 2) & (block <= 4), F32(1.0), F32(0.0))
    y_join(joined, (), (1.0, take_low, 1.0, take_high))
    lane, _, _, _ = place_of(0)
    for out, first in ((down, 1), (up, 2)):
        total_value = None
        for q in range(4):
            part = roll(joined[slice(128 * q, 128 * q + 128), :], 32 * (q - first))
            total_value = part if q == 0 else jnp.where(lane >> 5 == q, part, total_value)
        out[...] = total_value


def spread_kernel(joined, below, above, diag_up, diag_down, full, up, down):
    lane, block, _, _ = place_of(0)
    for q in range(4):
        at = slice(128 * q, 128 * q + 128)
        full[at, :] = jnp.where(
            lane < 32,
            roll(below[...], -32 * q),
            jnp.where(lane >= 96, roll(above[...], 96 - 32 * q), joined[at, :]),
        )
    take_low = jnp.where((block == 2) | (block == 6), F32(1.0), F32(0.0))
    take_high = jnp.where((block == 1) | (block == 5), F32(1.0), F32(0.0))
    y_join(full, (), (1.0, take_low, 1.0, take_high))
    x_join(full, (), x_weights(False))
    route(up, down, slice(0, 64), face(full, (), 0), face(full, (), 7))
    route(up, down, slice(64, 128), diag_down[...], diag_up[...])


def diagonal_kernel(inv, inv_far, weighted, diag, up, down, weighted_far, diag_far):
    wc = weight_column()
    cols = columns(SQUARE)
    for a in range(8):
        for b in range(8):
            at = slice(64 * a + 8 * b, 64 * a + 8 * b + 8)
            scale = WEIGHTS[a] * WEIGHTS[b] * wc
            weighted[at] = scale * inv[at]
            weighted_far[at] = scale * inv_far[at]
    for src, out, bs in ((weighted, diag, range(8)), (weighted_far, diag_far, (0, 7))):
        for b in bs:
            got = mix(SQUARE, [src[slice(64 * a + 8 * b, 64 * a + 8 * b + 8)] for a in range(8)])
            for a in range(8):
                out[slice(64 * a + 8 * b, 64 * a + 8 * b + 8)] = got[a]
        for a in range(8):
            start = 64 * a
            got = mix(SQUARE, [src[slice(start + 8 * b, start + 8 * b + 8)] for b in range(8)], bs)
            for b, value in zip(bs, got):
                at = slice(start + 8 * b, start + 8 * b + 8)
                inner = mix_inner(cols, src, (), start + 8 * b)
                scale = mass_shift * WEIGHTS[a] * WEIGHTS[b]
                out[at] = out[at] + value + inner + scale * wc
    xw = x_weights(False)
    x_join(diag, (), xw)
    for b in (0, 7):
        low, high = slice(8 * b, 8 * b + 8), slice(448 + 8 * b, 448 + 8 * b + 8)
        f0, f7 = diag_far[low], diag_far[high]
        diag_far[low] = xw[0] * f0 + xw[1] * roll(f7, 1)
        diag_far[high] = xw[2] * f7 + xw[3] * roll(f0, -1)
    y_join_two(diag, diag_far, (), y_weights(0, False), None)
    up[...] = face(diag, (), 7)
    down[...] = face(diag, (), 0)


def z_sum(src, both, across, first_row, dst):
    zw = z_weights()
    low, high = arrived(both, across, slice(first_row, first_row + 64))
    dst[...] = src[...]
    set_face(dst, (), 0, face(src, (), 0) + jnp.where(zw[1] > 0, low, F32(0.0)))
    set_face(dst, (), 7, face(src, (), 7) + jnp.where(zw[3] > 0, high, F32(0.0)))


def operate(u, weighted, out, flux):
    cols = columns(DERIV)
    cols_t = columns(DERIV_T)
    _, _, _, y = place_of(0)
    inside = (y >= 0) & (y < 4 * lax.axis_size("gy"))
    wc = jnp.where(inside, weight_column(), F32(0.0))

    def along_a(b, carry):
        start = 8 * b
        at = [rows8(64 * a + start) for a in range(8)]
        slope = mix(DERIV, [u[at[a]] for a in range(8)])
        got = mix(DERIV_T, [weighted[at[a]] * slope[a] for a in range(8)])
        for a in range(8):
            out[at[a]] = got[a]
        return carry

    lax.fori_loop(0, 8, along_a, 0)

    for a in range(8):
        start = 64 * a
        at = [slice(start + 8 * b, start + 8 * b + 8) for b in range(8)]
        values = [u[at[b]] for b in range(8)]
        weights = [weighted[at[b]] for b in range(8)]
        slope = mix(DERIV, values)
        got = mix(DERIV_T, [weights[b] * slope[b] for b in range(8)])
        for b in range(8):
            flux[at[b]] = weights[b] * mix_inner(cols, u, (), start + 8 * b)
            scale = mass_shift * WEIGHTS[a] * WEIGHTS[b]
            out[at[b]] = out[at[b]] + (got[b] + (scale * wc) * values[b])

    def along_c(k, carry):
        at = rows8(8 * k)
        out[at] = out[at] + mix_inner(cols_t, flux, (), 8 * k)
        return carry

    lax.fori_loop(0, 64, along_c, 0, unroll=4)


def own_mask():
    _, block, ix, _ = place_of(0)
    gx = lax.axis_index("gx_0") * lax.axis_size("gx_1") + lax.axis_index("gx_1")
    return jnp.where((block >= 2) & (block <= 5) & ((ix >> 2) == gx), F32(1.0), F32(0.0))


def dot(left, right):
    def step(k, carry):
        at = rows8(8 * k)
        return carry + left[at] * right[at]

    return lax.fori_loop(0, 64, step, jnp.zeros((8, LANES), F32), unroll=8)


def operator_one_kernel(
    partial, below, above, diag, source, weighted,
    residual, inverse, first, local, out, up, down, sums, flux,
):
    z_sum(partial, below, above, 0, residual)
    z_sum(diag, below, above, 64, inverse)
    inverse[...] = 1.0 / inverse[...]
    first[...] = residual[...] * inverse[...]
    operate(first, weighted, local, flux)
    out[...] = local[...]
    x_join(out, (), x_weights(False))
    y_join(out, (), y_weights(0, False))
    route(up, down, slice(0, 64), face(out, (), 0), face(out, (), 7))
    sums[0] = dot(source, first)
    sums[1] = dot(local, first)


def operator_two_kernel(
    partial, below, above, inverse, weighted, local, sums,
    applied, second, out, up, down, totals, local_two, flux,
):
    z_sum(partial, below, above, 0, applied)
    second[...] = applied[...] * inverse[...]
    operate(second, weighted, local_two, flux)
    mask = own_mask()
    lane = lax.broadcasted_iota(jnp.int32, (1, LANES), 1)
    row = jnp.zeros((1, LANES), F32)
    for k, value in enumerate((sums[0], sums[1], dot(local, second), dot(local_two, second))):
        part = jnp.sum(mask * value, axis=0, keepdims=True)
        part = jnp.sum(part, axis=1, keepdims=True)
        row = jnp.where(lane == k, part, row)
    totals[...] = jnp.broadcast_to(row[None], totals.shape)
    out[...] = local_two[...]
    x_join(out, (), x_weights(False))
    y_join(out, (), y_weights(0, False))
    route(up, down, slice(0, 64), face(out, (), 0), face(out, (), 7))


def to_slots(place, ref, lead, out, k, scratch):
    for p in range(4):
        at = slice(128 * p, 128 * p + 128)
        scratch[:, at] = jnp.transpose(ref[lead + (at,)])
    gx = lax.axis_index("gx_0") * lax.axis_size("gx_1") + lax.axis_index("gx_1")
    for s in range(16):
        q = place[s]
        lane = (2 + q % 4) * 16 + 4 * gx + q // 4
        out[k, slice(s, s + 1), :] = scratch[pl.ds(lane, 1), :]


def advected_kernel(place, advected, out, scratch):
    for i in range(3):
        to_slots(place, advected, (i,), out, i, scratch)


def fields_kernel(place, left, right, out, scratch):
    to_slots(place, left, (), out, 0, scratch)
    to_slots(place, right, (), out, 1, scratch)


def last_kernel(place, partial, below, above, out, full, scratch):
    z_sum(partial, below, above, 0, full)
    to_slots(place, full, (), out, 0, scratch)


def gather_kernel(pieces, out):
    row = jnp.sum(pieces[...], axis=0)
    out[...] = jnp.broadcast_to(row[None], out.shape)


def final_kernel(pieces, early, late, last, pressure, residual):
    row = jnp.sum(pieces[...], axis=0)
    rho, curvature, cross, tail = (row[:, k : k + 1] for k in range(4))
    step = rho / curvature
    rho_next = step * step * cross - rho
    ratio = rho_next / rho
    step_next = rho_next / (
        curvature - 2.0 * step * cross + step * step * tail - ratio * ratio * curvature
    )
    keep = step + step_next * (1.0 + ratio)
    both = step_next * step
    pressure[...] = keep * early[1] - both * late[1]
    residual[...] = early[0] - keep * late[0] + both * last[0]


def call(kernel, outs, scratch=(), scalars=0, raw=0):
    def run(*args):
        vm = pl.BlockSpec(memory_space=pltpu.VMEM)
        sm = pl.BlockSpec(memory_space=pltpu.SMEM)
        hbm = pl.BlockSpec(memory_space=pltpu.MemorySpace.HBM)
        return pl.pallas_call(
            kernel,
            out_shape=tuple(jax.ShapeDtypeStruct(shape, F32) for shape in outs),
            in_specs=[sm] * scalars + [hbm] * raw + [vm] * (len(args) - scalars - raw),
            out_specs=tuple(vm for _ in outs),
            scratch_shapes=[pltpu.VMEM(shape, F32) for shape in scratch]
            + ([pltpu.SemaphoreType.DMA((raw,))] if raw else []),
            compiler_params=pltpu.CompilerParams(vmem_limit_bytes=16 * 1024 * 1024),
        )(*args)

    return run


def shift(values, axis, step):
    count = lax.axis_size(axis)
    pairs = [(i, i + step) for i in range(count) if 0 <= i + step < count]
    return lax.ppermute(values, axis, pairs)


def paired(near, other):
    count = lax.axis_size(GZ)
    links = [pair for i in range(1, count - 1, 2) for pair in ((i, i + 1), (i + 1, i))]
    across = lax.ppermute(other, GZ, links)
    both = lax.all_gather(near, "gz_1")
    return both, across


def along(axis, up, down):
    return shift(up, axis, 1), shift(down, axis, -1)


FULL = (PTS, LANES)
THREE = (3, PTS, LANES)
FACE = (64, LANES)


def step(velocity, inv_density, element_place):
    hbm = pltpu.MemorySpace.HBM
    by_slot = pltpu.with_memory_space_constraint(jnp.transpose(velocity, (0, 2, 1)), hbm)
    inv_slot = pltpu.with_memory_space_constraint(jnp.transpose(inv_density), hbm)
    block, up, down = call(
        pack_kernel, [(64, PTS), (60, PTS), (60, PTS)], [(3, 16, PTS), (16, PTS)], 1, 2
    )(element_place, by_slot, inv_slot)
    below, above = along("gy", up, down)
    middle = lax.all_gather(block, GX)
    sides = lax.all_gather(jnp.concatenate([below, above]), GX)
    vel, vel_far, rate, rate_far, up, down, inv, inv_far = call(
        first_kernel,
        [THREE, THREE, THREE, THREE, (256, LANES), (256, LANES), FULL, FULL],
        [(256, PTS)],
    )(middle, sides)
    below, above = paired(up, down)
    weighted, diag, diag_up, diag_down = call(
        diagonal_kernel, [FULL, FULL, FACE, FACE], [FULL, FULL]
    )(inv, inv_far)
    acc, rate, up, down = call(
        second_kernel, [THREE, THREE, (192, LANES), (192, LANES)], [THREE, THREE, THREE]
    )(vel, vel_far, rate, rate_far, below, above)
    for scale, send, rows in ((0.5 * time_step, send_faces, 192), (time_step, send_own_faces, 96)):
        below, above = paired(up, down)
        acc, rate, up, down = call(
            stage_kernel(scale, time_step / 3.0, send),
            [THREE, THREE, (rows, LANES), (rows, LANES)],
            [THREE],
        )(vel, acc, rate, below, above)
    below, above = paired(up, down)
    advected, source, up, down, joined = call(
        source_kernel, [THREE, FULL, (128, LANES), (128, LANES), FULL]
    )(acc, rate, below, above)
    below, above = along("gy", up, down)
    (advected_slots,) = call(advected_kernel, [(3, 16, PTS)], [(LANES, PTS)], 1)(
        element_place, advected
    )
    full, up, down = call(spread_kernel, [FULL, (128, LANES), (128, LANES)])(
        joined, below, above, diag_up, diag_down
    )
    below, above = paired(up, down)
    residual, inverse, first, local, partial, up, down, sums = call(
        operator_one_kernel, [FULL, FULL, FULL, FULL, FULL, FACE, FACE, (2, 8, LANES)], [FULL]
    )(full, below, above, diag, source, weighted)
    below, above = paired(up, down)
    (early,) = call(fields_kernel, [(2, 16, PTS)], [(LANES, PTS)], 1)(
        element_place, residual, first
    )
    applied, second, partial, up, down, totals = call(
        operator_two_kernel, [FULL, FULL, FULL, FACE, FACE, (lax.axis_size(PLANE), 1, LANES)], [FULL, FULL]
    )(partial, below, above, inverse, weighted, local, sums)
    below, above = paired(up, down)
    pieces = lax.all_to_all(totals, PLANE, 0, 0)
    count = lax.axis_size("gz_0")
    (pieces,) = call(gather_kernel, [(count, 1, LANES)])(pieces)
    (late,) = call(fields_kernel, [(2, 16, PTS)], [(LANES, PTS)], 1)(element_place, applied, second)
    (last,) = call(last_kernel, [(1, 16, PTS)], [FULL, (LANES, PTS)], 1)(
        element_place, partial, below, above
    )
    pieces = lax.all_to_all(pieces, "gz_0", 0, 0)
    pressure, residual = call(final_kernel, [(16, PTS), (16, PTS)])(pieces, early, late, last)
    return (
        jnp.transpose(advected_slots, (0, 2, 1)),
        jnp.transpose(pressure),
        jnp.transpose(residual),
    )


def solution(mesh):
    torus = Mesh(
        mesh.devices.reshape(2, 2, mesh.shape["gy"], -1, 2),
        ("gx_0", "gx_1", "gy", "gz_0", "gz_1"),
    )
    placed = (P(None, None, GX_GY_GZ), P(None, GX_GY_GZ), P(GX_GY_GZ))
    return jax.shard_map(
        step,
        mesh=torus,
        in_specs=placed,
        out_specs=(P(None, None, GX_GY_GZ), P(None, GX_GY_GZ), P(None, GX_GY_GZ)),
        check_vma=False,
    )
```

```python
import jax
import jax.numpy as jnp
from jax import lax
from jax.experimental import pallas as pl
from jax.experimental.pallas import tpu as pltpu
from jax.sharding import Mesh
from jax.sharding import PartitionSpec as P


GX = ("gx_0", "gx_1")
GZ = ("gz_0", "gz_1")
PLANE = ("gx_0", "gx_1", "gy", "gz_1")
GX_GY_GZ = ("gx_0", "gx_1", "gy", "gz_0", "gz_1")
F32 = jnp.float32
PTS = 512
LANES = 128

time_step = 0.03
mass_shift = 4.0
inner_nodes = (
    -0.8717401485096066,
    -0.5917001814331423,
    -0.2092992179024789,
    0.2092992179024789,
    0.5917001814331423,
    0.8717401485096066,
)


def legendre_seven(position):
    previous = 1.0
    current_value = position
    for degree_index in range(1, 7):
        following = (
            (2 * degree_index + 1) * position * current_value - degree_index * previous
        ) / (degree_index + 1)
        previous = current_value
        current_value = following
    return current_value


def tables():
    nodes = [-1.0] + list(inner_nodes) + [1.0]
    poly = [legendre_seven(node) for node in nodes]
    weights = [2.0 / (56.0 * value * value) for value in poly]
    deriv = [[0.0] * 8 for _ in range(8)]
    for i in range(8):
        for j in range(8):
            if i != j:
                deriv[i][j] = poly[i] / (poly[j] * (nodes[i] - nodes[j]))
    deriv[0][0] = -14.0
    deriv[7][7] = 14.0
    return weights, deriv


WEIGHTS, DERIV = tables()
DERIV_T = [[DERIV[j][i] for j in range(8)] for i in range(8)]
SQUARE = [[DERIV[j][i] ** 2 for j in range(8)] for i in range(8)]
MINUS = [[-DERIV[i][j] for j in range(8)] for i in range(8)]


def mix(matrix, values, which=range(8)):
    sign = 1.0 if matrix is SQUARE else -1.0
    plus = [values[j] + values[7 - j] for j in range(4)]
    minus = [values[j] - values[7 - j] for j in range(4)]
    done = {}
    for i in sorted({min(i, 7 - i) for i in which}):
        even = odd = None
        for j in range(4):
            p, q = matrix[i][j], matrix[i][7 - j]
            e, o = 0.5 * (p + q) * plus[j], 0.5 * (p - q) * minus[j]
            even = e if even is None else even + e
            odd = o if odd is None else odd + o
        done[i] = odd + even
        done[7 - i] = even - odd if sign > 0 else odd - even
    return [done[i] for i in which]


def columns(matrix):
    sub = lax.broadcasted_iota(jnp.int32, (8, LANES), 0)
    out = []
    for j in range(8):
        col = jnp.zeros((8, LANES), F32)
        for i in range(8):
            col = jnp.where(sub == i, F32(matrix[i][j]), col)
        out.append(col)
    return out


def weight_column():
    sub = lax.broadcasted_iota(jnp.int32, (8, LANES), 0)
    col = jnp.zeros((8, LANES), F32)
    for i in range(8):
        col = jnp.where(sub == i, F32(WEIGHTS[i]), col)
    return col


def rows8(start):
    return pl.ds(pl.multiple_of(start, 8), 8)


def mix_inner(cols, ref, lead, start):
    total_value = None
    for j in range(8):
        term = cols[j] * ref[lead + (pl.ds(start + j, 8, stride=0), slice(None))]
        total_value = term if total_value is None else total_value + term
    return total_value


def place_of(tile):
    lane = lax.broadcasted_iota(jnp.int32, (1, LANES), 1)
    block = lane >> 4
    if tile == 0:
        row = block + 2
    else:
        row = jnp.where(block == 0, 1, jnp.where(block == 1, 10, jnp.where(block == 2, 0, 11)))
    return lane, block, lane & 15, row + 4 * (lax.axis_index("gy") - 1)


def pair_weights(has_low, has_high, average):
    own, other = (0.5, 0.5) if average else (1.0, 1.0)
    return (
        jnp.where(has_low, F32(own), F32(1.0)),
        jnp.where(has_low, F32(other), F32(0.0)),
        jnp.where(has_high, F32(own), F32(1.0)),
        jnp.where(has_high, F32(other), F32(0.0)),
    )


def x_weights(average):
    _, _, ix, _ = place_of(0)
    return pair_weights(ix > 0, ix < 15, average)


def y_weights(tile, average):
    _, _, _, y = place_of(tile)
    return pair_weights(y > 0, y < 4 * lax.axis_size("gy") - 1, average)


def z_index():
    return lax.axis_index("gz_0") * lax.axis_size("gz_1") + lax.axis_index("gz_1")


def z_weights():
    z = jnp.full((1, LANES), z_index(), jnp.int32)
    return pair_weights(z > 0, z < lax.axis_size("gz_0") * lax.axis_size("gz_1") - 1, True)


def roll(x, shift):
    return pltpu.roll(x, shift % LANES, 1)


def x_join(ref, lead, w):
    low, high = lead + (slice(0, 64),), lead + (slice(448, 512),)
    f0, f7 = ref[low], ref[high]
    ref[low] = w[0] * f0 + w[1] * roll(f7, 1)
    ref[high] = w[2] * f7 + w[3] * roll(f0, -1)


def y_join(ref, lead, w):
    for a in range(8):
        low, high = lead + (slice(64 * a, 64 * a + 8),), lead + (slice(64 * a + 56, 64 * a + 64),)
        f0, f7 = ref[low], ref[high]
        ref[low] = w[0] * f0 + w[1] * roll(f7, 16)
        ref[high] = w[2] * f7 + w[3] * roll(f0, -16)


def y_join_two(ref, far, lead, w, far_w):
    _, block, _, _ = place_of(0)
    for a in range(8):
        low, high = lead + (slice(64 * a, 64 * a + 8),), lead + (slice(64 * a + 56, 64 * a + 64),)
        f0, f7, g0, g7 = ref[low], ref[high], far[low], far[high]
        below = jnp.where(block == 0, g7, roll(f7, 16))
        above = jnp.where(block == 7, roll(g0, -32), roll(f0, -16))
        ref[low] = w[0] * f0 + w[1] * below
        ref[high] = w[2] * f7 + w[3] * above
        if far_w is not None:
            below = jnp.where(block == 0, roll(g7, -32), roll(f7, 32))
            above = jnp.where(block == 0, f0, roll(g0, -32))
            far[low] = far_w[0] * g0 + far_w[1] * below
            far[high] = far_w[2] * g7 + far_w[3] * above


def odd_place():
    return lax.axis_index("gz_1")


def route(near, other, at, low, high):
    odd = jnp.full((1, LANES), odd_place(), jnp.int32) == 1
    near[at, :] = jnp.where(odd, low, high)
    other[at, :] = jnp.where(odd, high, low)


def arrived(both, across, at):
    odd = jnp.full((1, LANES), odd_place(), jnp.int32) == 1
    pair, link = both[1 - odd_place(), at, :], across[at, :]
    return jnp.where(odd, pair, link), jnp.where(odd, link, pair)


def face(ref, lead, c):
    return ref[lead + (pl.ds(c, 64, stride=8), slice(None))]


def set_face(ref, lead, c, value):
    ref[lead + (pl.ds(c, 64, stride=8), slice(None))] = value


def convect(i, v, vel, out, minus_cols):
    def along_a(b, carry):
        start = 8 * b
        got = mix(MINUS, [v[i, rows8(64 * a + start)] for a in range(8)])
        for a in range(8):
            at = rows8(64 * a + start)
            out[i, at] = vel[0, at] * got[a]
        return carry

    lax.fori_loop(0, 8, along_a, 0, unroll=8)

    def along_bc(a, carry):
        start = 64 * a
        got = mix(MINUS, [v[i, rows8(start + 8 * b)] for b in range(8)])
        for b in range(8):
            at = rows8(start + 8 * b)
            inner = mix_inner(minus_cols, v, (i,), start + 8 * b)
            out[i, at] = out[i, at] + (vel[1, at] * got[b] + vel[2, at] * inner)
        return carry

    lax.fori_loop(0, 8, along_bc, 0, unroll=4)


def convect_y_faces(i, v, vel, out, minus_cols):
    for b in (0, 7):
        got = mix(MINUS, [v[i, slice(64 * a + 8 * b, 64 * a + 8 * b + 8)] for a in range(8)])
        for a in range(8):
            at = slice(64 * a + 8 * b, 64 * a + 8 * b + 8)
            out[i, at] = vel[0, at] * got[a]

    def along_bc(a, carry):
        start = 64 * a
        got = mix(MINUS, [v[i, rows8(start + 8 * b)] for b in range(8)], (0, 7))
        for b, value in zip((0, 7), got):
            at = rows8(start + 8 * b)
            inner = mix_inner(minus_cols, v, (i,), start + 8 * b)
            out[i, at] = out[i, at] + (vel[1, at] * value + vel[2, at] * inner)
        return carry

    lax.fori_loop(0, 8, along_bc, 0, unroll=4)


def pack_kernel(place_hbm, vel_hbm, inv_hbm, out, up, down, vel, inv, place, sems):
    copies = [
        pltpu.make_async_copy(place_hbm, place, sems.at[2]),
        pltpu.make_async_copy(vel_hbm, vel, sems.at[0]),
        pltpu.make_async_copy(inv_hbm, inv, sems.at[1]),
    ]
    for copy in copies:
        copy.start()
    for copy in copies:
        copy.wait()

    def move(s, carry):
        q = place[s]
        r = (q % 4) * 4 + q // 4
        for i in range(3):
            out[pl.ds(16 * i + r, 1), :] = vel[i, pl.ds(s, 1), :]
        out[pl.ds(48 + r, 1), :] = inv[pl.ds(s, 1), :]
        return carry

    lax.fori_loop(0, 16, move, 0)
    for ref, first in ((up, 52), (down, 48)):
        ref[0:48, :] = out[0:48, :]
        ref[48:60, :] = out[slice(first, first + 12), :]


FAR_ROWS = (1, 10, 0, 11)


def unpack(middle, sides, i, near, far, scratch, lead):
    for r in range(12):
        base = 16 * (r - 2) if 2 <= r <= 9 else LANES + 16 * FAR_ROWS.index(r)
        first = 16 * i + 4 * (r % 4)
        if r < 4 and i == 3:
            first -= 4
        if r >= 8:
            first += 60
        for g in range(4):
            at = slice(base + 4 * g, base + 4 * g + 4)
            if i == 3 and r in (0, 11):
                scratch[at, :] = jnp.zeros((4, PTS), F32)
            else:
                src = middle if 4 <= r < 8 else sides
                scratch[at, :] = src[g, slice(first, first + 4), :]
    for p in range(4):
        at = slice(128 * p, 128 * p + 128)
        near[lead + (at,)] = jnp.transpose(scratch[0:128, at])
        far[lead + (at,)] = jnp.transpose(scratch[128:256, at])


def first_kernel(middle, sides, vel, vel_far, rate, rate_far, up, down, inv, inv_far, scratch):
    scratch[192:256, :] = jnp.zeros((64, PTS), F32)
    for i in range(3):
        unpack(middle, sides, i, vel, vel_far, scratch, (i,))
    unpack(middle, sides, 3, inv, inv_far, scratch, ())
    minus_cols = columns(MINUS)
    xw = x_weights(True)
    yw = y_weights(0, True)
    fw = y_weights(1, True)

    def component(i, carry):
        convect(i, vel, vel, rate, minus_cols)
        convect(i, vel_far, vel_far, rate_far, minus_cols)
        x_join(rate, (i,), xw)
        x_join(rate_far, (i,), xw)
        y_join_two(rate, rate_far, (i,), yw, fw)
        return carry

    lax.fori_loop(0, 3, component, 0)
    lane, _, _, _ = place_of(0)
    for i in range(3):
        at = slice(64 * i, 64 * i + 64)
        route(up, down, at, face(rate, (i,), 0), face(rate, (i,), 7))
    ends = []
    for c in (0, 7):
        far = [face(rate_far, (i,), c) for i in range(3)]
        ends.append(
            jnp.where(lane < 32, far[0], jnp.where(lane < 64, roll(far[1], 32), roll(far[2], 64)))
        )
    route(up, down, slice(192, 256), *ends)


def advance(vel, rate, below, above, acc_in, scale, acc_scale, v, acc):
    zw = z_weights()

    def step(k, carry):
        at = rows8(8 * k)
        for i in range(3):
            r = rate[i, at]
            v[i, at] = vel[i, at] + scale * r
            if acc is not None:
                acc[i, at] = acc_in[i, at] + acc_scale * r
        return carry

    lax.fori_loop(0, 64, step, 0, unroll=8)
    for i in range(3):
        for c, got, own, other in ((0, below, zw[0], zw[1]), (7, above, zw[2], zw[3])):
            k = own * face(rate, (i,), c) + other * got[i]
            set_face(v, (i,), c, face(vel, (i,), c) + scale * k)
            if acc is not None:
                set_face(acc, (i,), c, face(acc_in, (i,), c) + acc_scale * k)


def thirds(both, across):
    got = [arrived(both, across, slice(64 * i, 64 * i + 64)) for i in range(3)]
    return [pair[0] for pair in got], [pair[1] for pair in got]


def second_kernel(
    vel, vel_far, rate, rate_far, below, above, acc, out, up, down, v, v_far, out_far
):
    advance(
        vel, rate, *thirds(below, above), vel, 0.5 * time_step, time_step / 6.0, v, acc
    )
    far = arrived(below, above, slice(192, 256))
    far = [[roll(part, -32 * i) for i in range(3)] for part in far]
    advance(vel_far, rate_far, far[0], far[1], None, 0.5 * time_step, 0.0, v_far, None)
    minus_cols = columns(MINUS)
    xw = x_weights(True)
    yw = y_weights(0, True)

    def component(i, carry):
        convect(i, v, vel, out, minus_cols)
        convect_y_faces(i, v_far, vel_far, out_far, minus_cols)
        x_join(out, (i,), xw)
        x_join_faces(out_far, i, xw)
        y_join_two(out, out_far, (i,), yw, None)
        return carry

    lax.fori_loop(0, 3, component, 0)
    send_faces(out, up, down)


def x_join_faces(ref, i, w):
    for b in (0, 7):
        low, high = slice(8 * b, 8 * b + 8), slice(448 + 8 * b, 448 + 8 * b + 8)
        f0, f7 = ref[i, low], ref[i, high]
        ref[i, low] = w[0] * f0 + w[1] * roll(f7, 1)
        ref[i, high] = w[2] * f7 + w[3] * roll(f0, -1)


def send_faces(rate, near, other):
    for i in range(3):
        at = slice(64 * i, 64 * i + 64)
        route(near, other, at, face(rate, (i,), 0), face(rate, (i,), 7))


def send_own_faces(rate, near, other):
    lane, _, _, _ = place_of(0)
    ends = []
    for c in (0, 7):
        f = [face(rate, (i,), c) for i in range(3)]
        ends.append(
            (
                jnp.where(lane < 64, roll(f[0], -32), roll(f[1], 32)),
                jnp.where(lane < 64, roll(f[2][0:32], -32), roll(f[2][32:64], 32)),
            )
        )
    route(near, other, slice(0, 64), ends[0][0], ends[1][0])
    route(near, other, slice(64, 96), ends[0][1], ends[1][1])


def own_thirds(both, across):
    wide = arrived(both, across, slice(0, 64))
    rest = arrived(both, across, slice(64, 96))
    return [
        [
            roll(w, 32),
            roll(w, -32),
            jnp.concatenate([roll(r, 32), roll(r, -32)], axis=0),
        ]
        for w, r in zip(wide, rest)
    ]


def stage_kernel(scale, acc_scale, send):
    def kernel(vel, acc_in, rate, below, above, acc, out, up, down, v):
        advance(vel, rate, *thirds(below, above), acc_in, scale, acc_scale, v, acc)
        minus_cols = columns(MINUS)
        xw = x_weights(True)
        yw = y_weights(0, True)

        def component(i, carry):
            convect(i, v, vel, out, minus_cols)
            x_join(out, (i,), xw)
            y_join(out, (i,), yw)
            return carry

        lax.fori_loop(0, 3, component, 0)
        send(out, up, down)

    return kernel


def own_rows():
    _, block, _, _ = place_of(0)
    return block


def source_kernel(acc_in, rate, below, above, advected, source, up, down, joined):
    advance(acc_in, rate, *own_thirds(below, above), None, time_step / 6.0, 0.0, advected, None)
    cols = columns(DERIV)
    wc = weight_column()

    def along_a(b, carry):
        start = 8 * b
        got = mix(DERIV, [advected[0, rows8(64 * a + start)] for a in range(8)])
        for a in range(8):
            source[rows8(64 * a + start)] = got[a]
        return carry

    lax.fori_loop(0, 8, along_a, 0, unroll=8)
    for a in range(8):
        start = 64 * a
        got = mix(DERIV, [advected[1, slice(start + 8 * b, start + 8 * b + 8)] for b in range(8)])
        for b in range(8):
            at = slice(start + 8 * b, start + 8 * b + 8)
            inner = mix_inner(cols, advected, (2,), start + 8 * b)
            scale = -WEIGHTS[a] * WEIGHTS[b] / time_step
            source[at] = (source[at] + got[b] + inner) * (scale * wc)
    joined[...] = source[...]
    block = own_rows()
    take_low = jnp.where((block >= 3) & (block <= 5), F32(1.0), F32(0.0))
    take_high = jnp.where((block >= 2) & (block <= 4), F32(1.0), F32(0.0))
    y_join(joined, (), (1.0, take_low, 1.0, take_high))
    lane, _, _, _ = place_of(0)
    for out, first in ((down, 1), (up, 2)):
        total_value = None
        for q in range(4):
            part = roll(joined[slice(128 * q, 128 * q + 128), :], 32 * (q - first))
            total_value = part if q == 0 else jnp.where(lane >> 5 == q, part, total_value)
        out[...] = total_value


def spread_kernel(joined, below, above, diag_up, diag_down, full, up, down):
    lane, block, _, _ = place_of(0)
    for q in range(4):
        at = slice(128 * q, 128 * q + 128)
        full[at, :] = jnp.where(
            lane < 32,
            roll(below[...], -32 * q),
            jnp.where(lane >= 96, roll(above[...], 96 - 32 * q), joined[at, :]),
        )
    take_low = jnp.where((block == 2) | (block == 6), F32(1.0), F32(0.0))
    take_high = jnp.where((block == 1) | (block == 5), F32(1.0), F32(0.0))
    y_join(full, (), (1.0, take_low, 1.0, take_high))
    x_join(full, (), x_weights(False))
    route(up, down, slice(0, 64), face(full, (), 0), face(full, (), 7))
    route(up, down, slice(64, 128), diag_down[...], diag_up[...])


def diagonal_kernel(inv, inv_far, weighted, diag, up, down, weighted_far, diag_far):
    wc = weight_column()
    cols = columns(SQUARE)
    for a in range(8):
        for b in range(8):
            at = slice(64 * a + 8 * b, 64 * a + 8 * b + 8)
            scale = WEIGHTS[a] * WEIGHTS[b] * wc
            weighted[at] = scale * inv[at]
            weighted_far[at] = scale * inv_far[at]
    for src, out, bs in ((weighted, diag, range(8)), (weighted_far, diag_far, (0, 7))):
        for b in bs:
            got = mix(SQUARE, [src[slice(64 * a + 8 * b, 64 * a + 8 * b + 8)] for a in range(8)])
            for a in range(8):
                out[slice(64 * a + 8 * b, 64 * a + 8 * b + 8)] = got[a]
        for a in range(8):
            start = 64 * a
            got = mix(SQUARE, [src[slice(start + 8 * b, start + 8 * b + 8)] for b in range(8)], bs)
            for b, value in zip(bs, got):
                at = slice(start + 8 * b, start + 8 * b + 8)
                inner = mix_inner(cols, src, (), start + 8 * b)
                scale = mass_shift * WEIGHTS[a] * WEIGHTS[b]
                out[at] = out[at] + value + inner + scale * wc
    xw = x_weights(False)
    x_join(diag, (), xw)
    for b in (0, 7):
        low, high = slice(8 * b, 8 * b + 8), slice(448 + 8 * b, 448 + 8 * b + 8)
        f0, f7 = diag_far[low], diag_far[high]
        diag_far[low] = xw[0] * f0 + xw[1] * roll(f7, 1)
        diag_far[high] = xw[2] * f7 + xw[3] * roll(f0, -1)
    y_join_two(diag, diag_far, (), y_weights(0, False), None)
    up[...] = face(diag, (), 7)
    down[...] = face(diag, (), 0)


def z_sum(src, both, across, first_row, dst):
    zw = z_weights()
    low, high = arrived(both, across, slice(first_row, first_row + 64))
    dst[...] = src[...]
    set_face(dst, (), 0, face(src, (), 0) + jnp.where(zw[1] > 0, low, F32(0.0)))
    set_face(dst, (), 7, face(src, (), 7) + jnp.where(zw[3] > 0, high, F32(0.0)))


def operate(u, weighted, out, flux):
    cols = columns(DERIV)
    cols_t = columns(DERIV_T)
    _, _, _, y = place_of(0)
    inside = (y >= 0) & (y < 4 * lax.axis_size("gy"))
    wc = jnp.where(inside, weight_column(), F32(0.0))

    def along_a(b, carry):
        start = 8 * b
        at = [rows8(64 * a + start) for a in range(8)]
        slope = mix(DERIV, [u[at[a]] for a in range(8)])
        got = mix(DERIV_T, [weighted[at[a]] * slope[a] for a in range(8)])
        for a in range(8):
            out[at[a]] = got[a]
        return carry

    lax.fori_loop(0, 8, along_a, 0, unroll=8)

    for a in range(8):
        start = 64 * a
        at = [slice(start + 8 * b, start + 8 * b + 8) for b in range(8)]
        values = [u[at[b]] for b in range(8)]
        weights = [weighted[at[b]] for b in range(8)]
        slope = mix(DERIV, values)
        got = mix(DERIV_T, [weights[b] * slope[b] for b in range(8)])
        for b in range(8):
            flux[at[b]] = weights[b] * mix_inner(cols, u, (), start + 8 * b)
            scale = mass_shift * WEIGHTS[a] * WEIGHTS[b]
            out[at[b]] = out[at[b]] + (got[b] + (scale * wc) * values[b])

    def along_c(k, carry):
        at = rows8(8 * k)
        out[at] = out[at] + mix_inner(cols_t, flux, (), 8 * k)
        return carry

    lax.fori_loop(0, 64, along_c, 0, unroll=16)


def own_mask():
    _, block, ix, _ = place_of(0)
    gx = lax.axis_index("gx_0") * lax.axis_size("gx_1") + lax.axis_index("gx_1")
    return jnp.where((block >= 2) & (block <= 5) & ((ix >> 2) == gx), F32(1.0), F32(0.0))


def dot(left, right):
    def step(k, carry):
        at = rows8(8 * k)
        return carry + left[at] * right[at]

    return lax.fori_loop(0, 64, step, jnp.zeros((8, LANES), F32), unroll=8)


def operator_one_kernel(
    partial, below, above, diag, source, weighted,
    residual, inverse, first, local, out, up, down, sums, flux,
):
    z_sum(partial, below, above, 0, residual)
    z_sum(diag, below, above, 64, inverse)
    inverse[...] = 1.0 / inverse[...]
    first[...] = residual[...] * inverse[...]
    operate(first, weighted, local, flux)
    out[...] = local[...]
    x_join(out, (), x_weights(False))
    y_join(out, (), y_weights(0, False))
    route(up, down, slice(0, 64), face(out, (), 0), face(out, (), 7))
    sums[0] = dot(source, first)
    sums[1] = dot(local, first)


def operator_two_kernel(
    partial, below, above, inverse, weighted, local, sums,
    applied, second, out, up, down, totals, local_two, flux,
):
    z_sum(partial, below, above, 0, applied)
    second[...] = applied[...] * inverse[...]
    operate(second, weighted, local_two, flux)
    mask = own_mask()
    lane = lax.broadcasted_iota(jnp.int32, (1, LANES), 1)
    row = jnp.zeros((1, LANES), F32)
    for k, value in enumerate((sums[0], sums[1], dot(local, second), dot(local_two, second))):
        part = jnp.sum(mask * value, axis=0, keepdims=True)
        part = jnp.sum(part, axis=1, keepdims=True)
        row = jnp.where(lane == k, part, row)
    totals[...] = jnp.broadcast_to(row[None], totals.shape)
    out[...] = local_two[...]
    x_join(out, (), x_weights(False))
    y_join(out, (), y_weights(0, False))
    route(up, down, slice(0, 64), face(out, (), 0), face(out, (), 7))


def to_slots(place, ref, lead, out, k, scratch):
    for p in range(4):
        at = slice(128 * p, 128 * p + 128)
        scratch[:, at] = jnp.transpose(ref[lead + (at,)])
    gx = lax.axis_index("gx_0") * lax.axis_size("gx_1") + lax.axis_index("gx_1")
    for s in range(16):
        q = place[s]
        lane = (2 + q % 4) * 16 + 4 * gx + q // 4
        out[k, slice(s, s + 1), :] = scratch[pl.ds(lane, 1), :]


def advected_kernel(place, advected, out, scratch):
    for i in range(3):
        to_slots(place, advected, (i,), out, i, scratch)


def fields_kernel(place, left, right, out, scratch):
    to_slots(place, left, (), out, 0, scratch)
    to_slots(place, right, (), out, 1, scratch)


def last_kernel(place, partial, below, above, out, full, scratch):
    z_sum(partial, below, above, 0, full)
    to_slots(place, full, (), out, 0, scratch)


def gather_kernel(pieces, out):
    row = jnp.sum(pieces[...], axis=0)
    out[...] = jnp.broadcast_to(row[None], out.shape)


def final_kernel(pieces, early, late, last, pressure, residual):
    row = jnp.sum(pieces[...], axis=0)
    rho, curvature, cross, tail = (row[:, k : k + 1] for k in range(4))
    step = rho / curvature
    rho_next = step * step * cross - rho
    ratio = rho_next / rho
    step_next = rho_next / (
        curvature - 2.0 * step * cross + step * step * tail - ratio * ratio * curvature
    )
    keep = step + step_next * (1.0 + ratio)
    both = step_next * step
    pressure[...] = keep * early[1] - both * late[1]
    residual[...] = early[0] - keep * late[0] + both * last[0]


def call(kernel, outs, scratch=(), scalars=0, raw=0):
    def run(*args):
        vm = pl.BlockSpec(memory_space=pltpu.VMEM)
        sm = pl.BlockSpec(memory_space=pltpu.SMEM)
        hbm = pl.BlockSpec(memory_space=pltpu.MemorySpace.HBM)
        return pl.pallas_call(
            kernel,
            out_shape=tuple(jax.ShapeDtypeStruct(shape, F32) for shape in outs),
            in_specs=[sm] * scalars + [hbm] * raw + [vm] * (len(args) - scalars - raw),
            out_specs=tuple(vm for _ in outs),
            scratch_shapes=[pltpu.VMEM(shape, F32) for shape in scratch]
            + ([pltpu.SMEM((16,), jnp.int32), pltpu.SemaphoreType.DMA((raw,))] if raw else []),
            compiler_params=pltpu.CompilerParams(vmem_limit_bytes=16 * 1024 * 1024),
        )(*args)

    return run


def shift(values, axis, step):
    count = lax.axis_size(axis)
    pairs = [(i, i + step) for i in range(count) if 0 <= i + step < count]
    return lax.ppermute(values, axis, pairs)


def paired(near, other):
    count = lax.axis_size(GZ)
    links = [pair for i in range(1, count - 1, 2) for pair in ((i, i + 1), (i + 1, i))]
    across = lax.ppermute(other, GZ, links)
    both = lax.all_gather(near, "gz_1")
    return both, across


def along(axis, up, down):
    return shift(up, axis, 1), shift(down, axis, -1)


FULL = (PTS, LANES)
THREE = (3, PTS, LANES)
FACE = (64, LANES)


def step(velocity, inv_density, element_place):
    hbm = pltpu.MemorySpace.HBM
    by_slot = pltpu.with_memory_space_constraint(jnp.transpose(velocity, (0, 2, 1)), hbm)
    inv_slot = pltpu.with_memory_space_constraint(jnp.transpose(inv_density), hbm)
    block, up, down = call(
        pack_kernel, [(64, PTS), (60, PTS), (60, PTS)], [(3, 16, PTS), (16, PTS)], 0, 3
    )(pltpu.with_memory_space_constraint(element_place, hbm), by_slot, inv_slot)
    below, above = along("gy", up, down)
    middle = lax.all_gather(block, GX)
    sides = lax.all_gather(jnp.concatenate([below, above]), GX)
    vel, vel_far, rate, rate_far, up, down, inv, inv_far = call(
        first_kernel,
        [THREE, THREE, THREE, THREE, (256, LANES), (256, LANES), FULL, FULL],
        [(256, PTS)],
    )(middle, sides)
    below, above = paired(up, down)
    weighted, diag, diag_up, diag_down = call(
        diagonal_kernel, [FULL, FULL, FACE, FACE], [FULL, FULL]
    )(inv, inv_far)
    acc, rate, up, down = call(
        second_kernel, [THREE, THREE, (192, LANES), (192, LANES)], [THREE, THREE, THREE]
    )(vel, vel_far, rate, rate_far, below, above)
    for scale, send, rows in ((0.5 * time_step, send_faces, 192), (time_step, send_own_faces, 96)):
        below, above = paired(up, down)
        acc, rate, up, down = call(
            stage_kernel(scale, time_step / 3.0, send),
            [THREE, THREE, (rows, LANES), (rows, LANES)],
            [THREE],
        )(vel, acc, rate, below, above)
    below, above = paired(up, down)
    advected, source, up, down, joined = call(
        source_kernel, [THREE, FULL, (128, LANES), (128, LANES), FULL]
    )(acc, rate, below, above)
    below, above = along("gy", up, down)
    (advected_slots,) = call(advected_kernel, [(3, 16, PTS)], [(LANES, PTS)], 1)(
        element_place, advected
    )
    full, up, down = call(spread_kernel, [FULL, (128, LANES), (128, LANES)])(
        joined, below, above, diag_up, diag_down
    )
    below, above = paired(up, down)
    residual, inverse, first, local, partial, up, down, sums = call(
        operator_one_kernel, [FULL, FULL, FULL, FULL, FULL, FACE, FACE, (2, 8, LANES)], [FULL]
    )(full, below, above, diag, source, weighted)
    below, above = paired(up, down)
    (early,) = call(fields_kernel, [(2, 16, PTS)], [(LANES, PTS)], 1)(
        element_place, residual, first
    )
    applied, second, partial, up, down, totals = call(
        operator_two_kernel, [FULL, FULL, FULL, FACE, FACE, (lax.axis_size(PLANE), 1, LANES)], [FULL, FULL]
    )(partial, below, above, inverse, weighted, local, sums)
    below, above = paired(up, down)
    pieces = lax.all_to_all(totals, PLANE, 0, 0)
    count = lax.axis_size("gz_0")
    (pieces,) = call(gather_kernel, [(count, 1, LANES)])(pieces)
    (late,) = call(fields_kernel, [(2, 16, PTS)], [(LANES, PTS)], 1)(element_place, applied, second)
    (last,) = call(last_kernel, [(1, 16, PTS)], [FULL, (LANES, PTS)], 1)(
        element_place, partial, below, above
    )
    pieces = lax.all_to_all(pieces, "gz_0", 0, 0)
    pressure, residual = call(final_kernel, [(16, PTS), (16, PTS)])(pieces, early, late, last)
    return (
        jnp.transpose(advected_slots, (0, 2, 1)),
        jnp.transpose(pressure),
        jnp.transpose(residual),
    )


def solution(mesh):
    torus = Mesh(
        mesh.devices.reshape(2, 2, mesh.shape["gy"], -1, 2),
        ("gx_0", "gx_1", "gy", "gz_0", "gz_1"),
    )
    placed = (P(None, None, GX_GY_GZ), P(None, GX_GY_GZ), P(GX_GY_GZ))
    return jax.shard_map(
        step,
        mesh=torus,
        in_specs=placed,
        out_specs=(P(None, None, GX_GY_GZ), P(None, GX_GY_GZ), P(None, GX_GY_GZ)),
        check_vma=False,
    )
```
